32 devices in a mesh: limb: 4 (over z), coef: 8 (over y, x, core).
Axes of the slice: x: 2, y: 2, z: 4, core: 2. Of those that a mesh axis runs over, the one named last changes fastest.
Arguments:
- residues: float32 [16, 64, 65536], P('limb', None, 'coef'), may hold values from 0 to 65534, as said below
- levels: int32 [64], replicated, may hold values from 1 to 16
- moduli: int32 [24], replicated, may hold values from 32768 to 65535, as said below
- inverse_table: int32 [16, 16], replicated, may hold values from 1 to 65534, as said below
- cross_table: int32 [16, 16, 8], replicated, may hold values from 0 to 65534, as said below
Outputs:
- source_part: float32 [16, 64, 65536], P('limb', 'coef')
- special_part: float32 [8, 64, 65536], P('limb', 'coef')
The draws below stay inside these ranges and needn't reach their ends.
Inputs may be any that keep to these rules, and one draw needn't show every extreme that they name: `moduli`: distinct primes; the first 16 form the source basis, the last 8 the special basis. `inverse_table`: entry [l, i] lies below the source modulus q_i. `cross_table`: entry [l, i, j] lies below the special modulus p_j. `residues`: whole numbers; entry [i, n, k] lies below the source modulus q_i.
All inputs are finite; a program needn't handle non-finite values.
Results may differ from the reference program's by a relative error of at most 0.0003.
Values may be sent and summed in bfloat16 or wider, within the bound.
No kernel may reach another device: no remote copies, remote signals or barrier semaphores. Data moves between devices by JAX's collectives and lax.ppermute only.
A program may use at most 192 MiB of HBM per device.

```python
import jax
import jax.numpy as jnp
from jax import lax

NCOEF = 65536
NQ = 16
NP = 8
CTS = 64


def prime_list():
    ceiling = 65536
    is_prime = [True] * ceiling
    is_prime[0] = False
    is_prime[1] = False
    for factor in range(2, 256):
        if is_prime[factor]:
            for multiple in range(factor * factor, ceiling, factor):
                is_prime[multiple] = False
    return [number for number in range(32768, ceiling) if is_prime[number]]


def chosen_moduli(key):
    primes = jnp.asarray(prime_list(), dtype=jnp.int32)
    shuffled = jax.random.permutation(jax.random.fold_in(key, 11), primes.shape[0])
    return primes[shuffled[:NQ + NP]]


def draw_moduli(key, part):
    return chosen_moduli(key)


def draw_inverse_table(key, part):
    bounds = chosen_moduli(key)[:NQ]
    return jax.random.randint(jax.random.fold_in(key, 12), (NQ, NQ), 1, bounds[None, :], dtype=jnp.int32)


def draw_cross_table(key, part):
    bounds = chosen_moduli(key)[NQ:]
    return jax.random.randint(jax.random.fold_in(key, 13), (NQ, NQ, NP), 0, bounds[None, None, :], dtype=jnp.int32)


def draw_residues(key, part):
    bounds = chosen_moduli(key)[:NQ][:, None, None]
    extent = (NQ, CTS, NCOEF)
    sample = jax.random.randint(jax.random.fold_in(key, 14), extent, 0, bounds, dtype=jnp.int32)
    return sample.astype(jnp.float32)


def plant(result, rng, low, high):
    shape = result.shape
    spot = [jax.random.randint(jax.random.fold_in(rng, axis), (), 0, shape[axis]) for axis in range(len(shape))]
    result = result.at[tuple(spot)].set(low)
    longest = shape.index(max(shape))
    spot[longest] = (spot[longest] + 1) % shape[longest]
    return result.at[tuple(spot)].set(high)


def setup_inputs(seed: int = 0) -> dict:
    key_list = jax.random.split(jax.random.key(seed), 6)
    return {
        "residues": draw_residues(jax.random.fold_in(key_list[5], 71), 0),
        "levels": plant(jax.random.randint(key_list[1], (CTS,), 1, NQ + 1), jax.random.fold_in(key_list[1], 1), 1, NQ).astype(jnp.int32),
        "moduli": draw_moduli(jax.random.fold_in(key_list[5], 71), 0),
        "inverse_table": draw_inverse_table(jax.random.fold_in(key_list[5], 71), 0),
        "cross_table": draw_cross_table(jax.random.fold_in(key_list[5], 71), 0),
    }


def modulo(amount, modulus):
    quotient = jnp.floor(amount / modulus)
    remain = amount - quotient * modulus
    remain = jnp.where(remain < 0, remain + modulus, remain)
    return jnp.where(remain >= modulus, remain - modulus, remain)


def split_bytes(amount):
    high_byte = jnp.floor(amount / 256.0)
    return amount - 256.0 * high_byte, high_byte


def level_tables(levels, inverse_table, cross_table):
    limb_total = inverse_table.shape[0]
    positions = jnp.arange(limb_total, dtype=jnp.int32)
    onehot = (levels[:, None] - 1 == positions[None, :]).astype(jnp.float32)
    inverse_rows = jnp.dot(onehot, inverse_table.astype(jnp.float32), precision=lax.Precision.HIGHEST)
    cross_rows = jnp.einsum("nl,lij->nij", onehot, cross_table.astype(jnp.float32), precision=lax.Precision.HIGHEST)
    active = (positions[None, :] < levels[:, None]).astype(jnp.float32)
    return inverse_rows, cross_rows, active


def scale_limbs(values, inverse_rows, active, source_mod):
    low_byte, high_byte = split_bytes(inverse_rows)
    modulus = source_mod[:, None, None]
    upper_part = modulo(values * high_byte[:, :, None], modulus)
    lower_part = modulo(values * low_byte[:, :, None], modulus)
    joined = modulo(modulo(256.0 * upper_part, modulus) + lower_part, modulus)
    return joined * active[:, :, None]


def fold_bytes(cross_rows, target_mod):
    modulus = target_mod[None, None, :]
    folded = jnp.stack([modulo(cross_rows, modulus), modulo(256.0 * cross_rows, modulus)], axis=3)
    low_byte, high_byte = split_bytes(folded)
    stacked = jnp.stack([low_byte, high_byte], axis=3)
    return jnp.transpose(stacked, (0, 2, 3, 1, 4)).astype(jnp.bfloat16)


def reduce_targets(digit_sums, modulus_row):
    modulus = modulus_row[:, None, None]
    upper_part = modulo(256.0 * modulo(digit_sums[:, 1], modulus), modulus)
    return modulo(upper_part + modulo(digit_sums[:, 0], modulus), modulus)


def reference(residues, levels, moduli, inverse_table, cross_table):
    module = moduli.astype(jnp.float32)
    source_mod = module[:NQ]
    target_mod = module[NQ:]
    inverse_rows, cross_rows, active = level_tables(levels, inverse_table, cross_table)
    source_part = residues * active.T[:, :, None] / source_mod[:, None, None]
    scaled = scale_limbs(residues, inverse_rows.T, active.T, source_mod)
    low_byte, high_byte = split_bytes(scaled)
    digits = jnp.stack([low_byte, high_byte], axis=1).astype(jnp.bfloat16)
    weights = fold_bytes(cross_rows, target_mod)
    digit_sums = jnp.einsum("lank,njbla->jbnk", digits.astype(jnp.float32), weights.astype(jnp.float32))
    converted = reduce_targets(digit_sums, target_mod)
    special_part = converted / target_mod[:, None, None]
    return source_part, special_part
```

```python
import functools

import jax
import jax.numpy as jnp
from jax import lax
from jax.experimental import pallas as pl
from jax.experimental.pallas import tpu as pltpu
from jax.sharding import PartitionSpec as P

LANES = 128
TILE = 2048


def modulo(amount, modulus):
    quotient = jnp.floor(amount / modulus)
    remain = amount - quotient * modulus
    remain = jnp.where(remain < 0, remain + modulus, remain)
    return jnp.where(remain >= modulus, remain - modulus, remain)


def split_bytes(amount):
    high_byte = jnp.floor(amount / 256.0)
    return (amount - 256.0 * high_byte, high_byte)


def pack_pair(first, second):
    return first | lax.shift_left(second, 16)


def halves(word):
    return word & 0xFFFF, lax.shift_right_logical(word, 16)


def centred(amount, modulus, inverse):
    return amount - jnp.round(amount * inverse) * modulus


def residue(amount, modulus, inverse):
    remain = centred(amount, modulus, inverse)
    return jnp.where(remain < 0, remain + modulus, remain)


def spread(column, width):
    return jnp.concatenate([column] * (width // LANES), axis=1)


def params(*semantics):
    return pltpu.CompilerParams(dimension_semantics=semantics)


def cost(elements, ops, moved):
    return pl.CostEstimate(flops=elements * ops, bytes_accessed=moved, transcendentals=0)


def pack_kernel(peers, values, *outs):
    turn = pl.program_id(0)
    width = values.shape[2]
    step = min(width, TILE)
    for place, out in enumerate(outs):

        @pl.when(turn == place)
        def _():
            for start in range(0, width, step):
                span = pl.ds(start, step)
                for word in range(out.shape[0]):
                    first = values[2 * word, :, span].astype(jnp.int32)
                    second = values[2 * word + 1, :, span].astype(jnp.int32)
                    out[word, :, span] = pack_pair(first, second)


def pack_blocks(residues, peers, block):
    limbs, _, width = residues.shape
    count = peers.shape[0]
    shape = (limbs // 2, block, width)
    return pl.pallas_call(
        pack_kernel,
        grid_spec=pltpu.PrefetchScalarGridSpec(
            num_scalar_prefetch=1,
            grid=(count,),
            in_specs=[pl.BlockSpec((limbs, block, width), lambda m, peers: (0, peers[m], 0))],
            out_specs=[pl.BlockSpec(shape, lambda m, peers: (0, 0, 0))] * count,
        ),
        out_shape=[jax.ShapeDtypeStruct(shape, jnp.int32)] * count,
        compiler_params=params("arbitrary"),
        cost_estimate=cost(count * limbs * block * width, 8, 6 * count * limbs * block * width),
        name="pack",
    )(peers, residues)


def scale_kernel(packed, place, source_rows, values, columns, *rest):
    source_out, scaled_out = rest[-2:]
    words, _, width = scaled_out.shape
    for word in range(words):
        if packed:
            pair = halves(values[word])
        else:
            pair = (values[2 * word], values[2 * word + 1])
        results = []
        for side, value in enumerate(pair):
            limb = 2 * word + side
            value = value.astype(jnp.float32)
            modulus, inverse = source_rows[0, limb], source_rows[1, limb]
            high, low, share = (spread(columns[kind, limb], width) for kind in range(3))
            source_out[limb] = value * share
            upper = centred(value * high, modulus, inverse)
            joined = residue(256.0 * upper + value * low, modulus, inverse)
            results.append(joined.astype(jnp.int32))
        scaled_out[word] = pack_pair(*results)


def scale_block(values, place, source_rows, columns, source_shape, source_buffer, scaled_shape, scaled_buffer, offset):
    packed = values.dtype == jnp.int32
    words, block, length = scaled_shape
    limbs = source_shape[0]
    width = source_shape[2] // place[1]
    tile = min(width, TILE)
    tiles = width // tile
    if packed:
        value_spec = pl.BlockSpec((words, block, tile), lambda i, place: (0, 0, i))
    else:
        value_spec = pl.BlockSpec((limbs, block, tile), lambda i, place: (0, place[0], i))
    in_specs = [
        pl.BlockSpec(memory_space=pltpu.SMEM),
        value_spec,
        pl.BlockSpec(columns.shape, lambda i, place: (0, 0, 0, 0)),
    ]
    operands = [place[0], source_rows, values, columns]
    aliases = {}
    for result, buffer in enumerate((source_buffer, scaled_buffer)):
        if buffer is not None:
            aliases[len(operands)] = result
            operands.append(buffer)
            in_specs.append(pl.BlockSpec(memory_space=pl.ANY))
    return pl.pallas_call(
        functools.partial(scale_kernel, packed),
        grid_spec=pltpu.PrefetchScalarGridSpec(
            num_scalar_prefetch=1,
            grid=(tiles,),
            in_specs=in_specs,
            out_specs=[
                pl.BlockSpec((limbs, block, tile), lambda i, place: (0, 0, place[0] * tiles + i)),
                pl.BlockSpec((words, block, tile), lambda i, place: (0, 0, offset * tiles + i)),
            ],
        ),
        out_shape=[
            jax.ShapeDtypeStruct(source_shape, jnp.float32),
            jax.ShapeDtypeStruct(scaled_shape, jnp.int32),
        ],
        input_output_aliases=aliases,
        compiler_params=params("arbitrary"),
        cost_estimate=cost(limbs * block * width, 40, 8 * limbs * block * width),
        name="scale",
    )(*operands)


def mix_kernel(target_rows, weights, own, received, far_out, outer_out, mine_out):
    digits = []
    for words in (own, received):
        for word in range(words.shape[0]):
            value = words[word]
            for byte in range(4):
                part = lax.shift_right_logical(value, 8 * byte) if byte else value
                if byte < 3:
                    part = part & 0xFF
                digits.append(part.astype(jnp.float32))
    stacked = jnp.concatenate(digits, axis=0).astype(jnp.bfloat16)
    sums = jnp.dot(weights[...], stacked, preferred_element_type=jnp.float32)
    block = own.shape[1]
    targets = sums.shape[0] // (2 * block)
    reduced = []
    for target in range(targets):
        modulus, inverse = target_rows[0, target], target_rows[1, target]
        low = sums[2 * target * block : (2 * target + 1) * block]
        high = sums[(2 * target + 1) * block : (2 * target + 2) * block]
        upper = centred(high, modulus, inverse)
        reduced.append(residue(256.0 * upper + low, modulus, inverse).astype(jnp.int32))
    words = [pack_pair(reduced[t], reduced[t + 1]) for t in range(0, targets, 2)]
    position = 0
    for out in (far_out, outer_out, mine_out):
        for word in range(out.shape[0]):
            out[word] = words[position]
            position += 1


def mix_chunk(own, received, weights, target_rows):
    words, block, length = own.shape
    tile = min(length, TILE)
    targets = target_rows.shape[1]
    quarter = targets // 8
    counts = (2 * quarter, quarter, quarter)
    spec = lambda count: pl.BlockSpec((count, block, tile), lambda i: (0, 0, i))
    return pl.pallas_call(
        mix_kernel,
        grid=(length // tile,),
        in_specs=[
            pl.BlockSpec(memory_space=pltpu.SMEM),
            pl.BlockSpec(weights.shape, lambda i: (0, 0)),
            spec(words),
            spec(words),
        ],
        out_specs=[spec(count) for count in counts],
        out_shape=[jax.ShapeDtypeStruct((count, block, length), jnp.int32) for count in counts],
        compiler_params=params("arbitrary"),
        cost_estimate=cost(targets * block * length, 40, 4 * (2 * words + 4) * block * length),
        name="mix",
    )(target_rows, weights, own, received)


def join_residues(first, second, modulus):
    total = first + second
    less = total - modulus
    return jnp.where(less < 0, total, less)


def forward_kernel(moduli, outer, arrived, out):
    for word in range(out.shape[0]):
        pairs = zip(halves(outer[word]), halves(arrived[word]))
        out[word] = pack_pair(*(join_residues(a, b, moduli[2 * word + side]) for side, (a, b) in enumerate(pairs)))


def forward_chunk(outer, arrived, moduli):
    words, block, length = outer.shape
    tile = min(length, 2 * TILE)
    spec = lambda first: pl.BlockSpec((words, block, tile), lambda i: (first, 0, i))
    return pl.pallas_call(
        forward_kernel,
        grid=(length // tile,),
        in_specs=[pl.BlockSpec(memory_space=pltpu.SMEM), spec(0), spec(1)],
        out_specs=spec(0),
        out_shape=jax.ShapeDtypeStruct(outer.shape, jnp.int32),
        compiler_params=params("arbitrary"),
        cost_estimate=cost(words * block * length, 40, 12 * words * block * length),
        name="forward",
    )(moduli, outer, arrived)


def finish_kernel(peers, inner, moduli, shares, mine, arrived, relayed, *rest):
    out = rest[-1]
    use_arrived = inner[0] > 0
    for word in range(mine.shape[0]):
        other = jnp.where(use_arrived, arrived[word], relayed[word])
        for side, (a, b) in enumerate(zip(halves(mine[word]), halves(other))):
            target = 2 * word + side
            total = join_residues(a, b, moduli[target])
            out[target] = total.astype(jnp.float32) * shares[target]


def finish_chunk(peers, first, inner, moduli, shares, mine, arrived, relayed, result_shape, buffer):
    words, block, length = mine.shape
    count = peers.shape[0]
    width = result_shape[2] // count
    tile = min(width, 2 * TILE)
    tiles = width // tile
    spec = pl.BlockSpec((words, block, tile), lambda b, i, peers: (0, 0, b * tiles + i))
    in_specs = [pl.BlockSpec(memory_space=pltpu.SMEM)] * 3 + [spec] * 3
    operands = [peers, inner, moduli, shares, mine, arrived, relayed]
    aliases = {}
    if buffer is not None:
        aliases[len(operands)] = 0
        operands.append(buffer)
        in_specs.append(pl.BlockSpec(memory_space=pl.ANY))
    return pl.pallas_call(
        finish_kernel,
        grid_spec=pltpu.PrefetchScalarGridSpec(
            num_scalar_prefetch=1,
            grid=(length // width, tiles),
            in_specs=in_specs,
            out_specs=pl.BlockSpec(
                (2 * words, block, tile), lambda b, i, peers: (0, 0, peers[first + b] * tiles + i)
            ),
        ),
        out_shape=jax.ShapeDtypeStruct(result_shape, jnp.float32),
        input_output_aliases=aliases,
        compiler_params=params("arbitrary", "arbitrary"),
        cost_estimate=cost(words * block * length, 40, 20 * words * block * length),
        name="finish",
    )(*operands)


def chunk_plan(count):
    unit = max(1, count // 8)
    sizes = [unit, unit, 2 * unit, 2 * unit]
    plan, start = [], 0
    for size in sizes:
        if start + size < count:
            plan.append(list(range(start, start + size)))
            start += size
    plan.append(list(range(start, count)))
    return plan


def per_device(residues, levels, moduli, inverse_table, cross_table):
    source_count = inverse_table.shape[0]
    limbs, _, width = residues.shape
    groups = lax.axis_size("limb")
    count = lax.axis_size("coef")
    target_count = cross_table.shape[2]
    own_targets = target_count // groups
    block = residues.shape[1] // count
    group = lax.axis_index("limb")
    home = lax.axis_index("coef")
    neighbour = group ^ 1
    inner = (group == 1) | (group == 2)
    left = group < 2

    module = moduli.astype(jnp.float32)
    own_levels = lax.dynamic_slice_in_dim(levels, home * block, block, 0)
    positions = jnp.arange(source_count, dtype=jnp.int32)
    onehot = (own_levels[:, None] - 1 == positions[None, :]).astype(jnp.float32)
    inverse_rows = jnp.dot(onehot, inverse_table.astype(jnp.float32), precision=lax.Precision.HIGHEST)
    active = (positions[None, :] < own_levels[:, None]).astype(jnp.float32)
    own_inverse = lax.dynamic_slice_in_dim(inverse_rows * active, group * limbs, limbs, 1).T
    own_active = lax.dynamic_slice_in_dim(active, group * limbs, limbs, 1).T
    source_mod = lax.dynamic_slice_in_dim(module, group * limbs, limbs, 0)
    high = jnp.floor((own_inverse + 128.0) / 256.0)
    columns = jnp.stack([high, own_inverse - 256.0 * high, own_active / source_mod[:, None]])
    columns = jnp.broadcast_to(columns[:, :, :, None], columns.shape + (LANES,))
    source_rows = jnp.stack([source_mod, 1.0 / source_mod])

    order = jnp.stack([jnp.where(left, 2, 1), jnp.where(left, 3, 0), neighbour, group])
    target_ids = (order[:, None] * own_targets + jnp.arange(own_targets)[None, :]).reshape(-1)
    pick = (target_ids[None, :] == jnp.arange(target_count)[:, None]).astype(jnp.float32)
    target_mod = jnp.dot(module[source_count:], pick, precision=lax.Precision.HIGHEST)
    target_rows = jnp.stack([target_mod, 1.0 / target_mod])
    cross = jnp.einsum("nl,lij->nij", onehot, cross_table.astype(jnp.float32), precision=lax.Precision.HIGHEST)
    cross = jnp.einsum("nij,jt->nit", cross, pick, precision=lax.Precision.HIGHEST)
    near = lax.dynamic_slice_in_dim(cross, group * limbs, limbs, 1)
    from_outer = lax.dynamic_slice_in_dim(cross, neighbour * limbs, limbs, 1)
    keep = inner & (jnp.arange(target_count) // own_targets != 2)
    cross = jnp.stack([near, from_outer * keep[None, None, :].astype(jnp.float32)], axis=1)
    folded = jnp.stack([cross, modulo(256.0 * cross, target_mod)], axis=4)
    low_byte, high_byte = split_bytes(folded)
    weights = jnp.stack([low_byte, high_byte], axis=5)
    weights = jnp.transpose(weights, (3, 5, 0, 1, 2, 4))
    eye = jnp.eye(block, dtype=jnp.float32)
    weights = weights[..., None] * eye[None, None, :, None, None, None, :]
    weights = weights.reshape(2 * target_count * block, 4 * limbs * block).astype(jnp.bfloat16)

    target_whole = target_mod.astype(jnp.int32)
    outer_mod = target_whole[2 * own_targets : 3 * own_targets]
    mine_mod = target_whole[3 * own_targets :]
    mine_share = target_rows[1, 3 * own_targets :]
    inner_flag = inner.astype(jnp.int32).reshape(1)

    peers = home ^ jnp.arange(count, dtype=jnp.int32)
    source_shape = (limbs, block, width * count)
    result_shape = (own_targets, block, width * count)
    plan = chunk_plan(count)

    packed = pack_blocks(residues, peers[1:], block)
    arrived = [residues]
    for offset in range(1, count):
        arrived.append(lax.ppermute(packed[offset - 1], "coef", [(i, i ^ offset) for i in range(count)]))

    source, result = None, None
    for chunk in plan:
        scaled_shape = (limbs // 2, block, width * len(chunk))
        scaled = None
        for offset, place in enumerate(chunk):
            source, scaled = scale_block(
                arrived[place],
                (peers[place : place + 1], count),
                source_rows,
                columns,
                source_shape,
                source,
                scaled_shape,
                scaled,
                offset,
            )
        received = lax.ppermute(scaled, "limb", [(0, 1), (3, 2)])
        far, outer, mine = mix_chunk(scaled, received, weights, target_rows)
        crossed = lax.ppermute(far, "limb", [(1, 2), (2, 1)])
        relay = forward_chunk(outer, crossed, outer_mod)
        relayed = lax.ppermute(relay, "limb", [(1, 0), (2, 3)])
        result = finish_chunk(
            peers, chunk[0], inner_flag, mine_mod, mine_share, mine, crossed, relayed, result_shape, result
        )
    return (source, result)


def solution(mesh):
    placed = (P("limb", None, "coef"), P(), P(), P(), P())
    return jax.shard_map(
        per_device,
        mesh=mesh,
        in_specs=placed,
        out_specs=(P("limb", "coef", None), P("limb", "coef", None)),
        check_vma=False,
    )
```

```python
import functools

import jax
import jax.numpy as jnp
from jax import lax
from jax.experimental import pallas as pl
from jax.experimental.pallas import tpu as pltpu
from jax.sharding import PartitionSpec as P

LANES = 128
MIB = 1024 * 1024
HERE = pl.BlockSpec(memory_space=pltpu.VMEM)
FAR = pl.BlockSpec(memory_space=pl.ANY)
SCALARS = pl.BlockSpec(memory_space=pltpu.SMEM)


def log2(number):
    assert number & (number - 1) == 0
    return number.bit_length() - 1


def pack_pair(first, second):
    return first | lax.shift_left(second, 16)


def halves(word):
    return word & 0xFFFF, lax.shift_right_logical(word, 16)


def centred(amount, modulus, inverse):
    return amount - jnp.round(amount * inverse) * modulus


def residue(amount, modulus, inverse):
    remain = centred(amount, modulus, inverse)
    return jnp.where(remain < 0, remain + modulus, remain)


def join_residues(first, second, modulus):
    total = first + second
    less = total - modulus
    return jnp.where(less < 0, total, less)


def spread(column, width):
    return jnp.concatenate([column] * (width // LANES), axis=1)


def params(limit):
    return pltpu.CompilerParams(vmem_limit_bytes=limit * MIB)


def cost(elements, ops, moved):
    return pl.CostEstimate(flops=elements * ops, bytes_accessed=moved, transcendentals=0)


def loop(count, body):
    lax.fori_loop(0, count, lambda step, carry: (body(step), carry)[1], 0)


def span_of(step, tile):
    return pl.ds(pl.multiple_of(step * tile, tile), tile)


def constants(limit):
    return lambda number: jnp.full(limit, number, jnp.int32).astype(jnp.float32)


def build_tables(place, levels, moduli, inverse, cross, columns, targets, weights):
    group, home = place[0], place[1]
    limbs, block = columns.shape[1], columns.shape[2]
    source_count = inverse.shape[0]
    total = targets.shape[1]
    quarter = total // 4
    shape = (block, LANES)
    fill = constants(shape)
    row = lax.broadcasted_iota(jnp.int32, shape, 0)
    own_levels = [levels[home * block + n] for n in range(block)]
    for limb in range(limbs):
        index = group * limbs + limb
        picked = jnp.zeros(shape, jnp.int32)
        live = jnp.zeros(shape, jnp.int32)
        for n, level in enumerate(own_levels):
            active = jnp.where(index < level, 1, 0)
            picked = jnp.where(row == n, inverse[level - 1, index] * active, picked)
            live = jnp.where(row == n, active, live)
        picked = picked.astype(jnp.float32)
        high = jnp.floor((picked + 128.0) * (1.0 / 256.0))
        modulus = fill(moduli[index])
        columns[0, limb] = high
        columns[1, limb] = picked - 256.0 * high
        columns[2, limb] = live.astype(jnp.float32) / modulus
        columns[3, limb] = modulus
        columns[4, limb] = 1.0 / modulus

    left = group < 2
    inner = (group == 1) | (group == 2)
    order = (jnp.where(left, 2, 1), jnp.where(left, 3, 0), group ^ 1, group)
    entries = cross.shape[1]
    lane = lax.broadcasted_iota(jnp.int32, (block, source_count), 1)
    rank = lax.broadcasted_iota(jnp.int32, (block, source_count), 0)
    level_rank = jnp.zeros((block, source_count), jnp.int32)
    for n, level in enumerate(own_levels):
        level_rank = jnp.where(rank == n, level - 1, level_rank)
    onehot = jnp.where(lane == level_rank, 1.0, 0.0).astype(jnp.bfloat16)
    table = cross[...]
    low = (table & 0xFF).astype(jnp.float32).astype(jnp.bfloat16)
    high = lax.shift_right_logical(table, 8).astype(jnp.float32).astype(jnp.bfloat16)
    low = jnp.dot(onehot, low, preferred_element_type=jnp.float32)
    high = jnp.dot(onehot, high, preferred_element_type=jnp.float32)
    target_of = lax.broadcasted_iota(jnp.int32, (block, entries), 1) & (total - 1)
    rows = []
    for target in range(total):
        index = order[target // quarter] * quarter + target % quarter
        for part in (low, high):
            rows.append(jnp.where(target_of == index, part, 0.0))
    width = weights.shape[1]
    entry = lax.broadcasted_iota(jnp.int32, (entries, width), 0)
    column = lax.broadcasted_iota(jnp.int32, (entries, width), 1)
    received = lax.shift_right_logical(column, log2(2 * block * limbs))
    limb = lax.shift_right_logical(column, log2(2 * block)) & (limbs - 1)
    limb = limb + jnp.where(received == 0, group * limbs, (group ^ 1) * limbs)
    choose = jnp.where(lax.shift_right_logical(entry, log2(total)) == limb, 1.0, 0.0).astype(jnp.bfloat16)
    stacked = jnp.concatenate(rows, axis=0).astype(jnp.bfloat16)
    chosen = jnp.dot(stacked, choose, preferred_element_type=jnp.float32)
    column = lax.broadcasted_iota(jnp.int32, (block, width), 1)
    same = (column & (block - 1)) == lax.broadcasted_iota(jnp.int32, (block, width), 0)
    upper = (lax.shift_right_logical(column, log2(block)) & 1) == 1
    from_outer = lax.shift_right_logical(column, log2(2 * block * limbs)) == 1
    results = []
    for target in range(total):
        index = order[target // quarter] * quarter + target % quarter
        modulus = fill(moduli[source_count + index])
        inverse_modulus = 1.0 / modulus
        targets[0, target] = modulus
        targets[1, target] = inverse_modulus
        modulus, inverse_modulus = spread(modulus, width), spread(inverse_modulus, width)
        first = 2 * target * block
        value = chosen[first : first + block] + 256.0 * chosen[first + block : first + 2 * block]
        value = jnp.where(upper, residue(256.0 * value, modulus, inverse_modulus), value)
        use = jnp.where(inner, 1, 0) if target // quarter != 2 else 0
        value = jnp.where(same & ((from_outer == False) | (use > 0)), value, 0.0)
        high_byte = jnp.floor(value * (1.0 / 256.0))
        results += [value - 256.0 * high_byte, high_byte]
    weights[...] = jnp.concatenate(results, axis=0).astype(jnp.bfloat16)


def scale_tile(values, columns, stage, scaled, read, write):
    width = write.size
    for word in range(scaled.shape[0]):
        if values.dtype == jnp.int32:
            pair = halves(values[word, :, read])
        else:
            pair = (values[2 * word, :, read], values[2 * word + 1, :, read])
        results = []
        for side, value in enumerate(pair):
            limb = 2 * word + side
            value = value.astype(jnp.float32)
            high, low, share, modulus, inverse = (spread(columns[kind, limb], width) for kind in range(5))
            stage[limb, :, read] = value * share
            upper = centred(value * high, modulus, inverse)
            results.append(residue(256.0 * upper + value * low, modulus, inverse).astype(jnp.int32))
        scaled[word, :, write] = pack_pair(*results)


def out_copy(stage, out, start, step, tile, sem):
    return pltpu.make_async_copy(
        stage.at[:, :, span_of(step, tile)],
        out.at[:, :, pl.ds(pl.multiple_of(start + step * tile, tile), tile)],
        sem.at[step],
    )


def first_kernel(
    place, levels, moduli, inverse, cross, residues, columns, targets, weights, source, scaled, landing, stage, sems, out_sems
):
    _, block, width = stage.shape
    tile = width // sems.shape[0]
    home = place[1]

    def load(step):
        return pltpu.make_async_copy(
            residues.at[:, pl.ds(pl.multiple_of(home * block, block), block), span_of(step, tile)],
            landing.at[:, :, span_of(step, tile)],
            sems.at[step],
        )

    def store(step):
        return out_copy(stage, source, home * width, step, tile, out_sems)

    steps = width // tile
    loop(steps, lambda step: load(step).start())
    build_tables(place, levels, moduli, inverse, cross, columns, targets, weights)

    def body(step):
        load(step).wait()
        scale_tile(landing, columns, stage, scaled, span_of(step, tile), span_of(step, tile))
        store(step).start()

    loop(steps, body)
    loop(steps, lambda step: store(step).wait())


def tile_of(width):
    return min(width, 1024)


def first(place, levels, moduli, inverse_table, cross, residues, block, count):
    limbs, _, width = residues.shape
    source_count = inverse_table.shape[0]
    total = moduli.shape[0] - source_count
    steps = width // tile_of(width)
    return pl.pallas_call(
        first_kernel,
        in_specs=[SCALARS] * 4 + [HERE, FAR],
        out_specs=[HERE, HERE, HERE, FAR, HERE],
        out_shape=[
            pltpu.VMEM((5, limbs, block, LANES), jnp.float32),
            pltpu.VMEM((2, total, block, LANES), jnp.float32),
            pltpu.VMEM((2 * total * block, 4 * limbs * block), jnp.bfloat16),
            jax.ShapeDtypeStruct((limbs, block, width * count), jnp.float32),
            pltpu.VMEM((limbs // 2, block, width), jnp.int32),
        ],
        scratch_shapes=[
            pltpu.VMEM((limbs, block, width), jnp.float32),
            pltpu.VMEM((limbs, block, width), jnp.float32),
            pltpu.SemaphoreType.DMA((steps,)),
            pltpu.SemaphoreType.DMA((steps,)),
        ],
        compiler_params=params(8),
        cost_estimate=cost(limbs * block * width, 60, 10 * limbs * block * width),
        name="first",
    )(place, levels, moduli, inverse_table, cross, residues)


def pack_kernel(offsets, place, residues, *rest):
    outs, (landing, sems) = rest[:-2], rest[-2:]
    _, _, block, width = landing.shape
    tile = tile_of(width)

    def load(turn):
        peer = place[1] ^ offsets[turn]
        return pltpu.make_async_copy(
            residues.at[:, pl.ds(pl.multiple_of(peer * block, block), block), :], landing.at[turn], sems.at[turn]
        )

    for turn in range(len(outs)):
        load(turn).start()
    for turn, out in enumerate(outs):
        load(turn).wait()

        def body(step):
            span = span_of(step, tile)
            for word in range(out.shape[0]):
                one = landing[turn, 2 * word, :, span].astype(jnp.int32)
                two = landing[turn, 2 * word + 1, :, span].astype(jnp.int32)
                out[word, :, span] = pack_pair(one, two)

        loop(width // tile, body)


def pack_blocks(place, residues, offsets, block):
    limbs, _, width = residues.shape
    peers = len(offsets)
    return pl.pallas_call(
        functools.partial(pack_kernel, offsets),
        in_specs=[SCALARS, FAR],
        out_specs=[HERE] * peers,
        out_shape=[pltpu.VMEM((limbs // 2, block, width), jnp.int32)] * peers,
        scratch_shapes=[
            pltpu.VMEM((peers, limbs, block, width), jnp.float32),
            pltpu.SemaphoreType.DMA((peers,)),
        ],
        compiler_params=params(12),
        cost_estimate=cost(peers * limbs * block * width, 16, 6 * peers * limbs * block * width),
        name="pack",
    )(place, residues)


def scale_kernel(offsets, place, columns, *rest):
    values = rest[: len(offsets)]
    source, scaled, stage, sems = rest[len(offsets) + 1 :]
    width = values[0].shape[2]
    tile = tile_of(width)
    steps = width // tile
    stores = []
    for turn, offset in enumerate(offsets):
        start = (place[1] ^ offset) * width

        def store(step, turn=turn, start=start):
            return out_copy(stage.at[turn], source, start, step, tile, sems.at[turn])

        def body(step):
            write = pl.ds(pl.multiple_of(turn * width + step * tile, tile), tile)
            scale_tile(values[turn], columns, stage.at[turn], scaled, span_of(step, tile), write)
            store(step).start()

        loop(steps, body)
        stores.append(store)
    for store in stores:
        loop(steps, lambda step: store(step).wait())


def scale_chunk(place, columns, values, offsets, source):
    words, block, width = values[0].shape
    limbs = source.shape[0]
    parts = len(values)
    return pl.pallas_call(
        functools.partial(scale_kernel, offsets),
        in_specs=[SCALARS, HERE] + [HERE] * parts + [FAR],
        out_specs=[FAR, HERE],
        out_shape=[
            jax.ShapeDtypeStruct(source.shape, jnp.float32),
            pltpu.VMEM((words, block, width * parts), jnp.int32),
        ],
        scratch_shapes=[
            pltpu.VMEM((parts, limbs, block, width), jnp.float32),
            pltpu.SemaphoreType.DMA((parts, width // tile_of(width))),
        ],
        input_output_aliases={2 + parts: 0},
        compiler_params=params(8),
        cost_estimate=cost(parts * limbs * block * width, 40, 8 * parts * limbs * block * width),
        name="scale",
    )(place, columns, *values, source)


def mix_kernel(targets, weights, own, received, far_out, outer_out, mine_out):
    block = own.shape[1]
    tile = tile_of(own.shape[2])

    def body(step):
        span = span_of(step, tile)
        digits = []
        for words in (own, received):
            for word in range(words.shape[0]):
                value = words[word, :, span]
                for byte in range(4):
                    part = lax.shift_right_logical(value, 8 * byte) if byte else value
                    if byte < 3:
                        part = part & 0xFF
                    digits.append(part.astype(jnp.float32))
        stacked = jnp.concatenate(digits, axis=0).astype(jnp.bfloat16)
        sums = jnp.dot(weights[...], stacked, preferred_element_type=jnp.float32)
        reduced = []
        for target in range(targets.shape[1]):
            modulus, inverse = spread(targets[0, target], tile), spread(targets[1, target], tile)
            low = sums[2 * target * block : (2 * target + 1) * block]
            high = sums[(2 * target + 1) * block : (2 * target + 2) * block]
            upper = centred(high, modulus, inverse)
            reduced.append(residue(256.0 * upper + low, modulus, inverse).astype(jnp.int32))
        words = [pack_pair(reduced[t], reduced[t + 1]) for t in range(0, len(reduced), 2)]
        position = 0
        for out in (far_out, outer_out, mine_out):
            for word in range(out.shape[0]):
                out[word, :, span] = words[position]
                position += 1

    loop(own.shape[2] // tile, body)


def mix_chunk(own, received, weights, targets):
    words, block, length = own.shape
    total = targets.shape[1]
    counts = (total // 4, total // 8, total // 8)
    return pl.pallas_call(
        mix_kernel,
        in_specs=[HERE] * 4,
        out_specs=[HERE] * 3,
        out_shape=[pltpu.VMEM((count, block, length), jnp.int32) for count in counts],
        compiler_params=params(8),
        cost_estimate=cost(total * block * length, 40, 4 * (2 * words + 4) * block * length),
        name="mix",
    )(targets, weights, own, received)


def forward_kernel(first_target, moduli, outer, arrived, out):
    words = out.shape[0]
    tile = tile_of(out.shape[2])

    def body(step):
        span = span_of(step, tile)
        for word in range(words):
            pairs = zip(halves(outer[word, :, span]), halves(arrived[words + word, :, span]))
            out[word, :, span] = pack_pair(
                *(
                    join_residues(a, b, spread(moduli[0, first_target + 2 * word + side].astype(jnp.int32), tile))
                    for side, (a, b) in enumerate(pairs)
                )
            )

    loop(out.shape[2] // tile, body)


def forward_chunk(outer, arrived, targets):
    words, block, length = outer.shape
    return pl.pallas_call(
        functools.partial(forward_kernel, 4 * words),
        in_specs=[HERE] * 3,
        out_specs=HERE,
        out_shape=pltpu.VMEM(outer.shape, jnp.int32),
        compiler_params=params(4),
        cost_estimate=cost(words * block * length, 40, 12 * words * block * length),
        name="forward",
    )(targets, outer, arrived)


def finish_kernel(offsets, first_target, place, targets, mine, arrived, relayed, *rest):
    out, stage, sems = rest[-3:]
    width = stage.shape[2] // len(offsets)
    tile = tile_of(width)
    steps = width // tile
    inner = (place[0] == 1) | (place[0] == 2)

    def store(step, turn):
        return pltpu.make_async_copy(
            stage.at[:, :, pl.ds(turn * width + step * tile, tile)],
            out.at[:, :, pl.ds(pl.multiple_of((place[1] ^ offsets[turn]) * width + step * tile, tile), tile)],
            sems.at[turn, step],
        )

    for turn in range(len(offsets)):

        def body(step):
            span = pl.ds(pl.multiple_of(turn * width + step * tile, tile), tile)
            for word in range(mine.shape[0]):
                other = jnp.where(inner, arrived[word, :, span], relayed[word, :, span])
                for side, (a, b) in enumerate(zip(halves(mine[word, :, span]), halves(other))):
                    target = first_target + 2 * word + side
                    modulus = spread(targets[0, target].astype(jnp.int32), tile)
                    total = join_residues(a, b, modulus).astype(jnp.float32)
                    stage[2 * word + side, :, span] = total * spread(targets[1, target], tile)
            store(step, turn).start()

        loop(steps, body)
    for turn in range(len(offsets)):
        loop(steps, lambda step: store(step, turn).wait())


def finish_chunk(place, targets, mine, arrived, relayed, offsets, shape, buffer):
    words, block, length = mine.shape
    width = length // len(offsets)
    operands = [place, targets, mine, arrived, relayed]
    in_specs = [SCALARS] + [HERE] * 4
    aliases = {}
    if buffer is not None:
        aliases[len(operands)] = 0
        operands.append(buffer)
        in_specs.append(FAR)
    return pl.pallas_call(
        functools.partial(finish_kernel, offsets, 6 * words),
        in_specs=in_specs,
        out_specs=FAR,
        out_shape=jax.ShapeDtypeStruct(shape, jnp.float32),
        scratch_shapes=[
            pltpu.VMEM((2 * words, block, length), jnp.float32),
            pltpu.SemaphoreType.DMA((len(offsets), width // tile_of(width))),
        ],
        input_output_aliases=aliases,
        compiler_params=params(8),
        cost_estimate=cost(words * block * length, 40, 20 * words * block * length),
        name="finish",
    )(*operands)


def chunk_plan(count):
    if count == 8:
        return [(0,), (1,), (2,), (4,), (3,), (5,), (6,), (7,)]
    unit = max(1, count // 8)
    edges = sorted({0, 1} | set(range(unit, count + 1, unit)))
    return [tuple(range(start, end)) for start, end in zip(edges, edges[1:])]


def timeline(plan):
    steps = len(plan)
    events = ["first", "a0", "pack"]
    order = [offset for chunk in plan for offset in chunk if offset]
    ready = [offset for chunk in plan[1:4] for offset in chunk]
    events += [f"p{offset}" for offset in ready]
    events += ["scale1", "a1"] + [f"p{offset}" for offset in order if offset not in ready]
    for step in range(steps + 3):
        if step < steps:
            events += [f"mix{step}", f"b{step}"]
        if step + 2 < steps:
            events += [f"scale{step + 2}", f"a{step + 2}"]
        if 1 <= step < steps + 1:
            events += [f"forward{step - 1}", f"c{step - 1}"]
        if 2 <= step < steps + 2:
            events.append(f"finish{step - 2}")
    return events


def per_device(residues, levels, moduli, inverse_table, cross_table):
    source_count, _, target_count = cross_table.shape
    _, _, width = residues.shape
    count = lax.axis_size("coef")
    assert lax.axis_size("limb") == 4
    block = residues.shape[1] // count
    place = jnp.stack([lax.axis_index("limb"), lax.axis_index("coef")]).astype(jnp.int32)
    residues = pltpu.with_memory_space_constraint(residues, pltpu.HBM)
    cross = cross_table.reshape(source_count, source_count * target_count)
    plan = chunk_plan(count)
    steps = len(plan)

    scaled, received, mixed, crossed, relayed = ([None] * steps for _ in range(5))
    arrived = {}
    packed = {}
    result = None
    shape = (target_count // 4, block, width * count)
    for event in timeline(plan):
        kind = event.rstrip("0123456789")
        step = int(event[len(kind) :] or 0)
        if kind == "first":
            columns, targets, weights, source, scaled[0] = first(
                place, levels, moduli, inverse_table, cross, residues, block, count
            )
        elif kind == "pack":
            offsets = tuple(range(1, count))
            packed = dict(zip(offsets, pack_blocks(place, residues, offsets, block)))
        elif kind == "p":
            arrived[step] = lax.ppermute(packed[step], "coef", [(i, i ^ step) for i in range(count)])
        elif kind == "scale":
            values = [arrived[offset] for offset in plan[step]]
            source, scaled[step] = scale_chunk(place, columns, values, plan[step], source)
        elif kind == "a":
            received[step] = lax.ppermute(scaled[step], "limb", [(0, 1), (3, 2)])
        elif kind == "mix":
            mixed[step] = mix_chunk(scaled[step], received[step], weights, targets)
        elif kind == "b":
            crossed[step] = lax.ppermute(mixed[step][0], "limb", [(1, 2), (2, 1)])
        elif kind == "forward":
            relayed[step] = forward_chunk(mixed[step][1], crossed[step], targets)
        elif kind == "c":
            relayed[step] = lax.ppermute(relayed[step], "limb", [(1, 0), (2, 3)])
        else:
            result = finish_chunk(
                place, targets, mixed[step][2], crossed[step], relayed[step], plan[step], shape, result
            )
    return (source, result)


def solution(mesh):
    placed = (P("limb", None, "coef"), P(), P(), P(), P())

    return jax.shard_map(
        per_device,
        mesh=mesh,
        in_specs=placed,
        out_specs=(P("limb", "coef", None), P("limb", "coef", None)),
        check_vma=False,
    )
```

```python
import functools

import jax
import jax.numpy as jnp
from jax import lax
from jax.experimental import pallas as pl
from jax.experimental.pallas import tpu as pltpu
from jax.sharding import PartitionSpec as P

LANES = 128
MIB = 1024 * 1024
HERE = pl.BlockSpec(memory_space=pltpu.VMEM)
FAR = pl.BlockSpec(memory_space=pl.ANY)
SCALARS = pl.BlockSpec(memory_space=pltpu.SMEM)


def log2(number):
    assert number & (number - 1) == 0
    return number.bit_length() - 1


def pack_pair(first, second):
    return first | lax.shift_left(second, 16)


def halves(word):
    return word & 0xFFFF, lax.shift_right_logical(word, 16)


def centred(amount, modulus, inverse):
    return amount - jnp.round(amount * inverse) * modulus


def residue(amount, modulus, inverse):
    remain = centred(amount, modulus, inverse)
    return jnp.where(remain < 0, remain + modulus, remain)


def join_residues(first, second, modulus):
    total = first + second
    less = total - modulus
    return jnp.where(less < 0, total, less)


def spread(column, width):
    return jnp.concatenate([column] * (width // LANES), axis=1)


def params(limit):
    return pltpu.CompilerParams(vmem_limit_bytes=limit * MIB)


def cost(elements, ops, moved):
    return pl.CostEstimate(flops=elements * ops, bytes_accessed=moved, transcendentals=0)


def loop(count, body):
    lax.fori_loop(0, count, lambda step, carry: (body(step), carry)[1], 0)


def span_of(step, tile):
    return pl.ds(pl.multiple_of(step * tile, tile), tile)


def constants(limit):
    return lambda number: jnp.full(limit, number, jnp.int32).astype(jnp.float32)


def build_tables(place, levels, moduli, inverse, cross, columns, targets, weights):
    group, home = place[0], place[1]
    limbs, block = columns.shape[1], columns.shape[2]
    source_count = inverse.shape[0]
    lane = lax.broadcasted_iota(jnp.int32, (block, source_count), 1)
    rank = lax.broadcasted_iota(jnp.int32, (block, source_count), 0)
    own_levels = [levels[home * block + n] for n in range(block)]
    level_rank = jnp.zeros((block, source_count), jnp.int32)
    for n, level in enumerate(own_levels):
        level_rank = jnp.where(rank == n, level - 1, level_rank)
    onehot = jnp.where(lane == level_rank, 1.0, 0.0).astype(jnp.bfloat16)

    def bytes_of(table):
        parts = (table & 0xFF, lax.shift_right_logical(table, 8))
        return [part.astype(jnp.float32).astype(jnp.bfloat16) for part in parts]

    def product(left, right):
        return jnp.dot(left, right, preferred_element_type=jnp.float32)

    inverse_low, inverse_high = (product(onehot, part) for part in bytes_of(inverse[...]))
    inverse_rows = jnp.where(lane <= level_rank, inverse_low + 256.0 * inverse_high, 0.0)
    live_rows = jnp.where(lane <= level_rank, 1.0, 0.0)
    total = targets.shape[1]
    quarter = total // 4
    shape = (block, LANES)
    fill = constants(shape)
    for limb in range(limbs):
        index = group * limbs + limb
        here = lane == index
        picked = jnp.sum(jnp.where(here, inverse_rows, 0.0), axis=1, keepdims=True)
        picked = jnp.broadcast_to(picked, shape)
        live = jnp.broadcast_to(jnp.sum(jnp.where(here, live_rows, 0.0), axis=1, keepdims=True), shape)
        high = jnp.floor((picked + 128.0) * (1.0 / 256.0))
        modulus = fill(moduli[index])
        columns[0, limb] = high
        columns[1, limb] = picked - 256.0 * high
        columns[2, limb] = live / modulus
        columns[3, limb] = modulus
        columns[4, limb] = 1.0 / modulus

    left = group < 2
    inner = (group == 1) | (group == 2)
    order = (jnp.where(left, 2, 1), jnp.where(left, 3, 0), group ^ 1, group)
    rows = []
    for target in range(total):
        index = order[target // quarter] * quarter + target % quarter
        rows += [product(onehot, part) for part in bytes_of(cross[:, index, :])]
    width = weights.shape[1]
    entry = lax.broadcasted_iota(jnp.int32, (source_count, width), 0)
    column = lax.broadcasted_iota(jnp.int32, (source_count, width), 1)
    received = lax.shift_right_logical(column, log2(2 * block * limbs))
    limb = lax.shift_right_logical(column, log2(2 * block)) & (limbs - 1)
    limb = limb + jnp.where(received == 0, group * limbs, (group ^ 1) * limbs)
    choose = jnp.where(entry == limb, 1.0, 0.0).astype(jnp.bfloat16)
    chosen = product(jnp.concatenate(rows, axis=0).astype(jnp.bfloat16), choose)
    column = lax.broadcasted_iota(jnp.int32, (block, width), 1)
    same = (column & (block - 1)) == lax.broadcasted_iota(jnp.int32, (block, width), 0)
    upper = (lax.shift_right_logical(column, log2(block)) & 1) == 1
    from_outer = lax.shift_right_logical(column, log2(2 * block * limbs)) == 1
    results = []
    for target in range(total):
        index = order[target // quarter] * quarter + target % quarter
        modulus = fill(moduli[source_count + index])
        inverse_modulus = 1.0 / modulus
        targets[0, target] = modulus
        targets[1, target] = inverse_modulus
        modulus, inverse_modulus = spread(modulus, width), spread(inverse_modulus, width)
        first = 2 * target * block
        value = chosen[first : first + block] + 256.0 * chosen[first + block : first + 2 * block]
        value = jnp.where(upper, residue(256.0 * value, modulus, inverse_modulus), value)
        use = jnp.where(inner, 1, 0) if target // quarter != 2 else 0
        value = jnp.where(same & ((from_outer == False) | (use > 0)), value, 0.0)
        high_byte = jnp.floor(value * (1.0 / 256.0))
        results += [value - 256.0 * high_byte, high_byte]
    weights[...] = jnp.concatenate(results, axis=0).astype(jnp.bfloat16)


def scale_tile(values, columns, stage, scaled, read, write, local):
    width = write.size
    for word in range(scaled.shape[0]):
        if values.dtype == jnp.int32:
            pair = halves(values[word, :, read])
        else:
            pair = (values[2 * word, :, read], values[2 * word + 1, :, read])
        results = []
        for side, value in enumerate(pair):
            limb = 2 * word + side
            value = value.astype(jnp.float32)
            high, low, share, modulus, inverse = (spread(columns[kind, limb], width) for kind in range(5))
            if stage is not None:
                stage[limb, :, local] = value * share
            upper = centred(value * high, modulus, inverse)
            results.append(residue(256.0 * upper + value * low, modulus, inverse).astype(jnp.int32))
        scaled[word, :, write] = pack_pair(*results)


def out_copy(stage, out, start, step, tile, sem):
    return pltpu.make_async_copy(
        stage.at[:, :, span_of(step, tile)],
        out.at[:, :, pl.ds(pl.multiple_of(start + step * tile, tile), tile)],
        sem.at[step],
    )


def first_kernel(place, *rest):
    tables, residues = rest[:4], rest[4]
    columns, targets, weights, source, scaled = rest[5:10]
    landing, stage, *copies = rest[10:-3]
    sems, out_sems, table_sems = rest[-3:]
    block, width = stage.shape[1:]
    tile = width // sems.shape[0]
    home = place[1]
    start = home * residues.shape[2]

    def load(step):
        return pltpu.make_async_copy(
            residues.at[:, pl.ds(pl.multiple_of(home * block, block), block), span_of(step, tile)],
            landing.at[:, :, span_of(step, tile)],
            sems.at[step],
        )

    def store(step):
        return out_copy(stage, source, start, step, tile, out_sems)

    steps = width // tile
    fetches = [pltpu.make_async_copy(a, b, table_sems.at[i]) for i, (a, b) in enumerate(zip(tables, copies))]
    for fetch in fetches:
        fetch.start()
    loop(steps, lambda step: load(step).start())
    for fetch in fetches:
        fetch.wait()
    build_tables(place, *copies, columns, targets, weights)

    def body(step):
        load(step).wait()
        span = span_of(step, tile)
        scale_tile(landing, columns, stage, scaled, span, span, span)
        store(step).start()

    loop(steps, body)
    loop(steps, lambda step: store(step).wait())


def tile_of(width):
    return min(width, 1024)


def first(place, levels, moduli, inverse_table, cross, residues, block, count, length):
    limbs, _, width = residues.shape
    source_count = inverse_table.shape[0]
    total = moduli.shape[0] - source_count
    steps = length // tile_of(length)
    return pl.pallas_call(
        first_kernel,
        in_specs=[SCALARS] + [FAR] * 5,
        out_specs=[HERE, HERE, HERE, FAR, HERE],
        out_shape=[
            pltpu.VMEM((5, limbs, block, LANES), jnp.float32),
            pltpu.VMEM((2, total, block, LANES), jnp.float32),
            pltpu.VMEM((2 * total * block, 4 * limbs * block), jnp.bfloat16),
            jax.ShapeDtypeStruct((limbs, block, width * count), jnp.float32),
            pltpu.VMEM((limbs // 2, block, length), jnp.int32),
        ],
        scratch_shapes=[
            pltpu.VMEM((limbs, block, length), jnp.float32),
            pltpu.VMEM((limbs, block, length), jnp.float32),
            pltpu.SMEM(levels.shape, jnp.int32),
            pltpu.SMEM(moduli.shape, jnp.int32),
            pltpu.VMEM(inverse_table.shape, jnp.int32),
            pltpu.VMEM(cross.shape, jnp.int32),
            pltpu.SemaphoreType.DMA((steps,)),
            pltpu.SemaphoreType.DMA((steps,)),
            pltpu.SemaphoreType.DMA((4,)),
        ],
        compiler_params=params(8),
        cost_estimate=cost(limbs * block * length, 60, 10 * limbs * block * length),
        name="first",
    )(place, *(far(x) for x in (levels, moduli, inverse_table, cross, residues)))


def far(array):
    return pltpu.with_memory_space_constraint(array, pltpu.HBM)


def pack_kernel(offsets, place, residues, *rest):
    outs, (landing, sems) = rest[:-2], rest[-2:]
    _, _, block, width = landing.shape
    tile = tile_of(width)

    def load(turn):
        peer = place[1] ^ offsets[turn]
        return pltpu.make_async_copy(
            residues.at[:, pl.ds(pl.multiple_of(peer * block, block), block), :], landing.at[turn], sems.at[turn]
        )

    for turn in range(len(outs)):
        load(turn).start()
    for turn, out in enumerate(outs):
        load(turn).wait()

        def body(step):
            span = span_of(step, tile)
            for word in range(out.shape[0]):
                one = landing[turn, 2 * word, :, span].astype(jnp.int32)
                two = landing[turn, 2 * word + 1, :, span].astype(jnp.int32)
                out[word, :, span] = pack_pair(one, two)

        loop(width // tile, body)


def pack_blocks(place, residues, offsets, block):
    limbs, _, width = residues.shape
    peers = len(offsets)
    return pl.pallas_call(
        functools.partial(pack_kernel, offsets),
        in_specs=[SCALARS, FAR],
        out_specs=[HERE] * peers,
        out_shape=[pltpu.VMEM((limbs // 2, block, width), jnp.int32)] * peers,
        scratch_shapes=[
            pltpu.VMEM((peers, limbs, block, width), jnp.float32),
            pltpu.SemaphoreType.DMA((peers,)),
        ],
        compiler_params=params(12),
        cost_estimate=cost(peers * limbs * block * width, 16, 6 * peers * limbs * block * width),
        name="pack",
    )(place, residues)


def scale_kernel(chunk, relay, emit, place, columns, targets, *rest):
    offsets, low, high = chunk
    values, rest = rest[: len(offsets)], rest[len(offsets) :]
    if relay:
        outer, arrived, *rest = rest
    if emit:
        source, scaled, *rest = rest[1:]
        stage, sems = rest[-2:]
    else:
        scaled, *rest = rest
    send = rest[0] if relay else None
    width = values[0].shape[2]
    length = high - low
    tile = tile_of(length)
    steps = length // tile
    inner = (place[0] == 1) | (place[0] == 2)
    stores = []
    for turn, offset in enumerate(offsets):
        start = (place[1] ^ offset) * width + low

        def store(step, turn=turn, start=start):
            return out_copy(stage.at[turn], source, start, step, tile, sems.at[turn])

        def body(step):
            write = pl.ds(pl.multiple_of(turn * length + step * tile, tile), tile)
            read = pl.ds(pl.multiple_of(low + step * tile, tile), tile)
            local = span_of(step, tile)
            scale_tile(values[turn], columns, stage.at[turn] if emit else None, scaled, read, write, local)
            if relay:
                for word in range(send.shape[0]):
                    words = scaled[word, :, write]
                    if word < outer.shape[0]:
                        words = jnp.where(inner, relay_word(targets, outer, arrived, word, write), words)
                    send[word, :, write] = words
            if emit:
                store(step).start()

        loop(steps, body)
        stores.append(store)
    if emit:
        for store in stores:
            loop(steps, lambda step: store(step).wait())


def scale_chunk(place, columns, targets, values, chunk, source, relay=None):
    words, block, _ = values[0].shape
    _, low, high = chunk
    length = high - low
    parts = len(values)
    limbs = 2 * words
    emit = source is not None
    operands = [place, columns, targets, *values, *(relay or ())]
    in_specs = [SCALARS] + [HERE] * (len(operands) - 1)
    whole = pltpu.VMEM((words, block, length * parts), jnp.int32)
    out_shape, out_specs, scratch, aliases = [whole], [HERE], [], {}
    if relay:
        out_shape, out_specs = out_shape + [whole], out_specs + [HERE]
    if emit:
        aliases = {len(operands): 0}
        operands.append(source)
        in_specs.append(FAR)
        out_shape = [jax.ShapeDtypeStruct(source.shape, jnp.float32)] + out_shape
        out_specs = [FAR] + out_specs
        scratch = [
            pltpu.VMEM((parts, limbs, block, length), jnp.float32),
            pltpu.SemaphoreType.DMA((parts, length // tile_of(length))),
        ]
    results = pl.pallas_call(
        functools.partial(scale_kernel, chunk, relay is not None, emit),
        in_specs=in_specs,
        out_specs=out_specs,
        out_shape=out_shape,
        scratch_shapes=scratch,
        input_output_aliases=aliases,
        compiler_params=params(8),
        cost_estimate=cost(parts * limbs * block * length, 40, 8 * parts * limbs * block * length),
        name="scale",
    )(*operands)
    if emit:
        source, *results = results
    scaled = results[0]
    return source, scaled, results[1] if relay else scaled


def spread_kernel(pieces, place, columns, *rest):
    values = rest[: len(pieces)]
    source, stage, sems = rest[-3:]
    tile = stage.shape[3]
    stores = []
    for turn, (offset, low, high, width) in enumerate(pieces):
        steps = (high - low) // tile
        base = sum((p[2] - p[1]) // tile for p in pieces[:turn])

        def store(step, base=base, offset=offset, low=low, width=width):
            return pltpu.make_async_copy(
                stage.at[base + step],
                source.at[:, :, pl.ds(pl.multiple_of((place[1] ^ offset) * width + low + step * tile, tile), tile)],
                sems.at[base + step],
            )

        def body(step):
            read = pl.ds(pl.multiple_of(low + step * tile, tile), tile)
            for word in range(values[turn].shape[0]):
                for side, value in enumerate(halves(values[turn][word, :, read])):
                    limb = 2 * word + side
                    stage[base + step, limb] = value.astype(jnp.float32) * spread(columns[2, limb], tile)
            store(step).start()

        loop(steps, body)
        stores.append((steps, store))
    for steps, store in stores:
        loop(steps, lambda step: store(step).wait())


def spread_blocks(place, columns, values, pieces, source):
    words, block, width = values[0].shape
    tile = min(tile_of(high - low) for _, low, high in pieces)
    pieces = tuple((offset, low, high, width) for offset, low, high in pieces)
    slots = sum((high - low) // tile for _, low, high, _ in pieces)
    operands = [place, columns, *values, source]
    return pl.pallas_call(
        functools.partial(spread_kernel, pieces),
        in_specs=[SCALARS] + [HERE] * (len(operands) - 2) + [FAR],
        out_specs=FAR,
        out_shape=jax.ShapeDtypeStruct(source.shape, jnp.float32),
        scratch_shapes=[
            pltpu.VMEM((slots, 2 * words, block, tile), jnp.float32),
            pltpu.SemaphoreType.DMA((slots,)),
        ],
        input_output_aliases={len(operands) - 1: 0},
        compiler_params=params(12),
        cost_estimate=cost(slots * 2 * words * block * tile, 20, 6 * slots * 2 * words * block * tile),
        name="spread",
    )(*operands)


def mix_kernel(targets, weights, own, received, far_out, outer_out, mine_out):
    block = own.shape[1]
    tile = min(own.shape[2], 2048)

    def body(step):
        span = span_of(step, tile)
        digits = []
        for words in (own, received):
            for word in range(words.shape[0]):
                value = words[word, :, span]
                for byte in range(4):
                    part = lax.shift_right_logical(value, 8 * byte) if byte else value
                    if byte < 3:
                        part = part & 0xFF
                    digits.append(part.astype(jnp.float32))
        stacked = jnp.concatenate(digits, axis=0).astype(jnp.bfloat16)
        sums = jnp.dot(weights[...], stacked, preferred_element_type=jnp.float32)
        reduced = []
        for target in range(targets.shape[1]):
            modulus, inverse = spread(targets[0, target], tile), spread(targets[1, target], tile)
            low = sums[2 * target * block : (2 * target + 1) * block]
            high = sums[(2 * target + 1) * block : (2 * target + 2) * block]
            upper = centred(high, modulus, inverse)
            reduced.append(residue(256.0 * upper + low, modulus, inverse).astype(jnp.int32))
        words = [pack_pair(reduced[t], reduced[t + 1]) for t in range(0, len(reduced), 2)]
        position = 0
        for out in (far_out, outer_out, mine_out):
            for word in range(out.shape[0]):
                out[word, :, span] = words[position]
                position += 1

    loop(own.shape[2] // tile, body)


def mix_chunk(own, received, weights, targets):
    words, block, length = own.shape
    total = targets.shape[1]
    counts = (total // 4, total // 8, total // 8)
    return pl.pallas_call(
        mix_kernel,
        in_specs=[HERE] * 4,
        out_specs=[HERE] * 3,
        out_shape=[pltpu.VMEM((count, block, length), jnp.int32) for count in counts],
        compiler_params=params(8),
        cost_estimate=cost(total * block * length, 40, 4 * (2 * words + 4) * block * length),
        name="mix",
    )(targets, weights, own, received)


def relay_word(targets, outer, arrived, word, span):
    words = outer.shape[0]
    results = []
    for side, (a, b) in enumerate(zip(halves(outer[word, :, span]), halves(arrived[words + word, :, span]))):
        modulus = spread(targets[0, 4 * words + 2 * word + side].astype(jnp.int32), span.size)
        results.append(join_residues(a, b, modulus))
    return pack_pair(*results)


def forward_kernel(targets, outer, arrived, out):
    tile = tile_of(out.shape[2])

    def body(step):
        span = span_of(step, tile)
        for word in range(out.shape[0]):
            out[word, :, span] = relay_word(targets, outer, arrived, word, span)

    loop(out.shape[2] // tile, body)


def forward_chunk(outer, arrived, targets):
    words, block, length = outer.shape
    return pl.pallas_call(
        forward_kernel,
        in_specs=[HERE] * 3,
        out_specs=HERE,
        out_shape=pltpu.VMEM(outer.shape, jnp.int32),
        compiler_params=params(4),
        cost_estimate=cost(words * block * length, 40, 12 * words * block * length),
        name="forward",
    )(targets, outer, arrived)


def finish_kernel(chunks, full, place, targets, *rest):
    out, stage, sems = rest[-3:]
    tile = stage.shape[3]
    inner = (place[0] == 1) | (place[0] == 2)
    stores = []
    slot = 0
    for turn, (offsets, low, high) in enumerate(chunks):
        mine, arrived, relayed = rest[3 * turn : 3 * turn + 3]
        first_target = 6 * mine.shape[0]
        steps = (high - low) // tile
        for part, offset in enumerate(offsets):

            def store(step, offset=offset, low=low, base=slot):
                start = (place[1] ^ offset) * full + low
                return pltpu.make_async_copy(
                    stage.at[base + step],
                    out.at[:, :, pl.ds(pl.multiple_of(start + step * tile, tile), tile)],
                    sems.at[base + step],
                )

            def body(step):
                span = pl.ds(pl.multiple_of(part * (high - low) + step * tile, tile), tile)
                for word in range(mine.shape[0]):
                    other = jnp.where(inner, arrived[word, :, span], relayed[word, :, span])
                    for side, (a, b) in enumerate(zip(halves(mine[word, :, span]), halves(other))):
                        target = first_target + 2 * word + side
                        modulus = spread(targets[0, target].astype(jnp.int32), tile)
                        total = join_residues(a, b, modulus).astype(jnp.float32)
                        stage[slot + step, 2 * word + side] = total * spread(targets[1, target], tile)
                store(step).start()

            loop(steps, body)
            stores.append((steps, store))
            slot += steps
    for steps, store in stores:
        loop(steps, lambda step: store(step).wait())


def finish_chunks(place, targets, triples, chunks, shape, full, buffer):
    words, block, _ = triples[0][0].shape
    tile = min(tile_of(high - low) for _, low, high in chunks)
    slots = sum(len(offsets) * (high - low) // tile for offsets, low, high in chunks)
    operands = [place, targets, *(array for triple in triples for array in triple)]
    in_specs = [SCALARS] + [HERE] * (len(operands) - 1)
    aliases = {}
    if buffer is not None:
        aliases[len(operands)] = 0
        operands.append(buffer)
        in_specs.append(FAR)
    return pl.pallas_call(
        functools.partial(finish_kernel, chunks, full),
        in_specs=in_specs,
        out_specs=FAR,
        out_shape=jax.ShapeDtypeStruct(shape, jnp.float32),
        scratch_shapes=[
            pltpu.VMEM((slots, 2 * words, block, tile), jnp.float32),
            pltpu.SemaphoreType.DMA((slots,)),
        ],
        input_output_aliases=aliases,
        compiler_params=params(8),
        cost_estimate=cost(2 * words * block * slots * tile, 20, 10 * 2 * words * block * slots * tile),
        name="finish",
    )(*operands)


def chunk_plan(count, width):
    if count == 8:
        return [((offset,), 0, width) for offset in (0, 1, 2, 4, 3, 5, 6, 7)]
    unit = max(1, count // 8)
    edges = sorted({0, 1} | set(range(unit, count + 1, unit)))
    return [(tuple(range(start, end)), 0, width) for start, end in zip(edges, edges[1:])]


LAG = 3
LATE = 4


def length_of(chunk):
    return len(chunk[0]) * (chunk[2] - chunk[1])


def riders(plan):
    return {
        step: step - LAG
        for step in range(LAG, len(plan))
        if length_of(plan[step]) == length_of(plan[step - LAG])
    }


def timeline(plan):
    steps = len(plan)
    ride = riders(plan)
    events = ["first", "a0", "pack"]
    order = list(dict.fromkeys(offset for chunk in plan for offset in chunk[0] if offset))
    ready = list(dict.fromkeys(offset for chunk in plan[:4] for offset in chunk[0] if offset))
    events += [f"p{offset}" for offset in ready]
    events += ["scale1", "a1"] + [f"p{offset}" for offset in order if offset not in ready]
    alone = [step for step in range(steps) if step not in ride.values()]
    for step in range(steps):
        events += [f"mix{step}", f"b{step}"]
        if step + 2 < steps:
            events += [f"scale{step + 2}", f"a{step + 2}"]
        if step - 1 in alone:
            events += [f"forward{step - 1}", f"c{step - 1}"]
    joined = [step for step in range(steps) if step not in alone]
    tail = steps - 1
    events[events.index(f"b{tail}") + 1 : events.index(f"b{tail}") + 1] = ["spread"]
    events += ["finish" + "_".join(map(str, joined + alone[:-2]))]
    events += [f"forward{tail}", f"c{tail}", f"finish{tail - 1}", f"finish{tail}"]
    return events


def late(plan):
    return set(range(len(plan) - LATE, len(plan)))


def per_device(residues, levels, moduli, inverse_table, cross_table):
    target_count = cross_table.shape[2]
    _, _, width = residues.shape
    count = lax.axis_size("coef")
    assert lax.axis_size("limb") == 4
    block = residues.shape[1] // count
    place = jnp.stack([lax.axis_index("limb"), lax.axis_index("coef")]).astype(jnp.int32)
    cross = jnp.transpose(cross_table, (0, 2, 1))
    plan = chunk_plan(count, width)
    steps = len(plan)
    ride = riders(plan)

    scaled, send, received, mixed, crossed, relayed = ([None] * steps for _ in range(6))
    arrived = {}
    packed = {}
    result = None
    shape = (target_count // 4, block, width * count)
    for event in timeline(plan):
        kind = event.rstrip("0123456789_")
        step = int(event[len(kind) :] or 0) if "_" not in event else 0
        if kind == "first":
            columns, targets, weights, source, scaled[0] = first(
                place, levels, moduli, inverse_table, cross, residues, block, count, plan[0][2]
            )
            send[0] = scaled[0]
        elif kind == "pack":
            offsets = tuple(range(1, count))
            packed = dict(zip(offsets, pack_blocks(place, far(residues), offsets, block)))
        elif kind == "p":
            arrived[step] = lax.ppermute(packed[step], "coef", [(i, i ^ step) for i in range(count)])
        elif kind == "scale":
            values = [arrived[offset] for offset in plan[step][0]]
            relay = (mixed[ride[step]][1], crossed[ride[step]]) if step in ride else None
            buffer = None if step in late(plan) else source
            buffer, scaled[step], send[step] = scale_chunk(place, columns, targets, values, plan[step], buffer, relay)
            source = source if step in late(plan) else buffer
        elif kind == "a":
            pairs = [(0, 1), (3, 2)] + ([(1, 0), (2, 3)] if step in ride else [])
            received[step] = lax.ppermute(send[step], "limb", pairs)
            if step in ride:
                relayed[ride[step]] = received[step]
        elif kind == "mix":
            mixed[step] = mix_chunk(scaled[step], received[step], weights, targets)
        elif kind == "b":
            crossed[step] = lax.ppermute(mixed[step][0], "limb", [(1, 2), (2, 1)])
        elif kind == "forward":
            relayed[step] = forward_chunk(mixed[step][1], crossed[step], targets)
        elif kind == "c":
            relayed[step] = lax.ppermute(relayed[step], "limb", [(1, 0), (2, 3)])
        elif kind == "spread":
            pieces = [(offset, low, high) for i in sorted(late(plan)) for offset, low, high in [(o, *plan[i][1:]) for o in plan[i][0]]]
            source = spread_blocks(place, columns, [arrived[p[0]] for p in pieces], pieces, source)
        else:
            chosen = [int(i) for i in event[len(kind) :].split("_")]
            triples = [(mixed[i][2], crossed[i], relayed[i]) for i in chosen]
            result = finish_chunks(
                place, targets, triples, tuple(plan[i] for i in chosen), shape, width, result
            )
    return (source, result)


def solution(mesh):
    placed = (P("limb", None, "coef"), P(), P(), P(), P())

    return jax.shard_map(
        per_device,
        mesh=mesh,
        in_specs=placed,
        out_specs=(P("limb", "coef", None), P("limb", "coef", None)),
        check_vma=False,
    )
```

```python
import functools

import jax
import jax.numpy as jnp
from jax import lax
from jax.experimental import pallas as pl
from jax.experimental.pallas import tpu as pltpu
from jax.sharding import PartitionSpec as P

LANES = 128
MIB = 1024 * 1024
HERE = pl.BlockSpec(memory_space=pltpu.VMEM)
FAR = pl.BlockSpec(memory_space=pl.ANY)
SCALARS = pl.BlockSpec(memory_space=pltpu.SMEM)


def log2(number):
    assert number & (number - 1) == 0
    return number.bit_length() - 1


def pack_pair(first, second):
    return first | lax.shift_left(second, 16)


def halves(word):
    return word & 0xFFFF, lax.shift_right_logical(word, 16)


def centred(amount, modulus, inverse):
    return amount - jnp.round(amount * inverse) * modulus


def residue(amount, modulus, inverse):
    remain = centred(amount, modulus, inverse)
    return jnp.where(remain < 0, remain + modulus, remain)


def join_residues(first, second, modulus):
    total = first + second
    less = total - modulus
    return jnp.where(less < 0, total, less)


def spread(column, width):
    return jnp.concatenate([column] * (width // LANES), axis=1)


def params(limit):
    return pltpu.CompilerParams(vmem_limit_bytes=limit * MIB)


def cost(elements, ops, moved):
    return pl.CostEstimate(flops=elements * ops, bytes_accessed=moved, transcendentals=0)


def loop(count, body):
    lax.fori_loop(0, count, lambda step, carry: (body(step), carry)[1], 0)


def span_of(step, tile):
    return pl.ds(pl.multiple_of(step * tile, tile), tile)


def constants(limit):
    return lambda number: jnp.full(limit, number, jnp.int32).astype(jnp.float32)


def product(left, right):
    return jnp.dot(left, right, preferred_element_type=jnp.float32)


def bytes_of(table):
    parts = (table & 0xFF, lax.shift_right_logical(table, 8))
    return [part.astype(jnp.float32).astype(jnp.bfloat16) for part in parts]


def level_rows(place, levels, block, source_count):
    lane = lax.broadcasted_iota(jnp.int32, (block, source_count), 1)
    rank = lax.broadcasted_iota(jnp.int32, (block, source_count), 0)
    level_rank = jnp.zeros((block, source_count), jnp.int32)
    for n in range(block):
        level_rank = jnp.where(rank == n, levels[place[1] * block + n] - 1, level_rank)
    return lane, level_rank, jnp.where(lane == level_rank, 1.0, 0.0).astype(jnp.bfloat16)


def build_columns(place, levels, moduli, inverse, columns):
    group = place[0]
    limbs, block = columns.shape[1], columns.shape[2]
    lane, level_rank, onehot = level_rows(place, levels, block, inverse.shape[0])
    inverse_low, inverse_high = (product(onehot, part) for part in bytes_of(inverse[...]))
    inverse_rows = jnp.where(lane <= level_rank, inverse_low + 256.0 * inverse_high, 0.0)
    live_rows = jnp.where(lane <= level_rank, 1.0, 0.0)
    shape = (block, LANES)
    fill = constants(shape)
    for limb in range(limbs):
        index = group * limbs + limb
        here = lane == index
        picked = jnp.sum(jnp.where(here, inverse_rows, 0.0), axis=1, keepdims=True)
        picked = jnp.broadcast_to(picked, shape)
        live = jnp.broadcast_to(jnp.sum(jnp.where(here, live_rows, 0.0), axis=1, keepdims=True), shape)
        high = jnp.floor((picked + 128.0) * (1.0 / 256.0))
        modulus = fill(moduli[index])
        columns[0, limb] = high
        columns[1, limb] = picked - 256.0 * high
        columns[2, limb] = live / modulus
        columns[3, limb] = modulus
        columns[4, limb] = 1.0 / modulus


def build_weights(place, levels, moduli, cross, limbs, targets, weights):
    group = place[0]
    total, block = targets.shape[1:3]
    source_count = cross.shape[0]
    quarter = total // 4
    fill = constants((block, LANES))
    onehot = level_rows(place, levels, block, source_count)[2]
    left = group < 2
    inner = (group == 1) | (group == 2)
    order = (jnp.where(left, 2, 1), jnp.where(left, 3, 0), group ^ 1, group)
    rows = []
    for target in range(total):
        index = order[target // quarter] * quarter + target % quarter
        rows += [product(onehot, part) for part in bytes_of(cross[:, index, :])]
    width = weights.shape[1]
    entry = lax.broadcasted_iota(jnp.int32, (source_count, width), 0)
    column = lax.broadcasted_iota(jnp.int32, (source_count, width), 1)
    received = lax.shift_right_logical(column, log2(2 * block * limbs))
    limb = lax.shift_right_logical(column, log2(2 * block)) & (limbs - 1)
    limb = limb + jnp.where(received == 0, group * limbs, (group ^ 1) * limbs)
    choose = jnp.where(entry == limb, 1.0, 0.0).astype(jnp.bfloat16)
    chosen = product(jnp.concatenate(rows, axis=0).astype(jnp.bfloat16), choose)
    column = lax.broadcasted_iota(jnp.int32, (block, width), 1)
    same = (column & (block - 1)) == lax.broadcasted_iota(jnp.int32, (block, width), 0)
    upper = (lax.shift_right_logical(column, log2(block)) & 1) == 1
    from_outer = lax.shift_right_logical(column, log2(2 * block * limbs)) == 1
    results = []
    for target in range(total):
        index = order[target // quarter] * quarter + target % quarter
        modulus = fill(moduli[source_count + index])
        inverse_modulus = 1.0 / modulus
        targets[0, target] = modulus
        targets[1, target] = inverse_modulus
        modulus, inverse_modulus = spread(modulus, width), spread(inverse_modulus, width)
        first = 2 * target * block
        value = chosen[first : first + block] + 256.0 * chosen[first + block : first + 2 * block]
        value = jnp.where(upper, residue(256.0 * value, modulus, inverse_modulus), value)
        use = jnp.where(inner, 1, 0) if target // quarter != 2 else 0
        value = jnp.where(same & ((from_outer == False) | (use > 0)), value, 0.0)
        high_byte = jnp.floor(value * (1.0 / 256.0))
        results += [value - 256.0 * high_byte, high_byte]
    weights[...] = jnp.concatenate(results, axis=0).astype(jnp.bfloat16)


def scale_tile(values, columns, stage, scaled, read, write, local):
    width = write.size
    for word in range(scaled.shape[0]):
        if values.dtype == jnp.int32:
            pair = halves(values[word, :, read])
        else:
            pair = (values[2 * word, :, read], values[2 * word + 1, :, read])
        results = []
        for side, value in enumerate(pair):
            limb = 2 * word + side
            value = value.astype(jnp.float32)
            high, low, share, modulus, inverse = (spread(columns[kind, limb], width) for kind in range(5))
            if stage is not None:
                stage[limb, :, local] = value * share
            upper = centred(value * high, modulus, inverse)
            results.append(residue(256.0 * upper + value * low, modulus, inverse).astype(jnp.int32))
        scaled[word, :, write] = pack_pair(*results)


def out_copy(stage, out, start, step, tile, sem):
    return pltpu.make_async_copy(
        stage.at[:, :, span_of(step, tile)],
        out.at[:, :, pl.ds(pl.multiple_of(start + step * tile, tile), tile)],
        sem.at[step],
    )


def first_kernel(place, *rest):
    tables, residues, columns, scaled, landing = rest[:3], *rest[3:7]
    copies, (sems, table_sems) = rest[7:-2], rest[-2:]
    block, width = landing.shape[1:]
    tile = width // sems.shape[0]

    def load(step):
        return pltpu.make_async_copy(
            residues.at[:, pl.ds(pl.multiple_of(place[1] * block, block), block), span_of(step, tile)],
            landing.at[:, :, span_of(step, tile)],
            sems.at[step],
        )

    steps = width // tile
    fetches = [pltpu.make_async_copy(a, b, table_sems.at[i]) for i, (a, b) in enumerate(zip(tables, copies))]
    for fetch in fetches:
        fetch.start()
    loop(steps, lambda step: load(step).start())
    for fetch in fetches:
        fetch.wait()
    build_columns(place, *copies, columns)

    def body(step):
        load(step).wait()
        span = span_of(step, tile)
        scale_tile(landing, columns, None, scaled, span, span, span)

    loop(steps, body)


def tile_of(width):
    return min(width, 1024)


def first(place, levels, moduli, inverse_table, residues, block, length):
    limbs = residues.shape[0]
    steps = length // tile_of(length)
    return pl.pallas_call(
        first_kernel,
        in_specs=[SCALARS] + [FAR] * 4,
        out_specs=[HERE, HERE],
        out_shape=[
            pltpu.VMEM((5, limbs, block, LANES), jnp.float32),
            pltpu.VMEM((limbs // 2, block, length), jnp.int32),
        ],
        scratch_shapes=[
            pltpu.VMEM((limbs, block, length), jnp.float32),
            pltpu.SMEM(levels.shape, jnp.int32),
            pltpu.SMEM(moduli.shape, jnp.int32),
            pltpu.VMEM(inverse_table.shape, jnp.int32),
            pltpu.SemaphoreType.DMA((steps,)),
            pltpu.SemaphoreType.DMA((3,)),
        ],
        compiler_params=params(8),
        cost_estimate=cost(limbs * block * length, 60, 10 * limbs * block * length),
        name="first",
    )(place, *(far(x) for x in (levels, moduli, inverse_table, residues)))


def far(array):
    return pltpu.with_memory_space_constraint(array, pltpu.HBM)


def pack_kernel(offsets, place, columns, levels, moduli, cross, residues, targets, weights, source, *rest):
    outs, (landing, stage, level_copy, moduli_copy, cross_copy, sems, own_sems, table_sems) = rest[:-8], rest[-8:]
    _, limbs, block, width = landing.shape
    tile = tile_of(width)

    def load(turn):
        peer = place[1] ^ offsets[turn]
        return pltpu.make_async_copy(
            residues.at[:, pl.ds(pl.multiple_of(peer * block, block), block), :], landing.at[turn], sems.at[turn]
        )

    fetches = [
        pltpu.make_async_copy(array, copy, table_sems.at[i])
        for i, (array, copy) in enumerate(((levels, level_copy), (moduli, moduli_copy), (cross, cross_copy)))
    ]
    for fetch in fetches:
        fetch.start()
    for turn in range(len(offsets)):
        load(turn).start()
    for fetch in fetches:
        fetch.wait()
    build_weights(place, level_copy, moduli_copy, cross_copy, limbs, targets, weights)

    def store(step):
        return out_copy(stage, source, place[1] * width, step, tile, own_sems)

    for turn, out in enumerate((None, *outs)):
        load(turn).wait()

        def body(step):
            span = span_of(step, tile)
            if out is None:
                for limb in range(limbs):
                    stage[limb, :, span] = landing[turn, limb, :, span] * spread(columns[2, limb], tile)
                store(step).start()
                return
            for word in range(limbs // 2):
                one = landing[turn, 2 * word, :, span].astype(jnp.int32)
                two = landing[turn, 2 * word + 1, :, span].astype(jnp.int32)
                out[word, :, span] = pack_pair(one, two)

        loop(width // tile, body)
    loop(width // tile, lambda step: store(step).wait())


def pack_blocks(place, columns, levels, moduli, cross, residues, block, count):
    limbs, _, width = residues.shape
    total, _ = cross.shape[1:]
    offsets = tuple(range(count))
    peers = count - 1
    results = pl.pallas_call(
        functools.partial(pack_kernel, offsets),
        in_specs=[SCALARS, HERE] + [FAR] * 4,
        out_specs=[HERE, HERE, FAR] + [HERE] * peers,
        out_shape=[
            pltpu.VMEM((2, total, block, LANES), jnp.float32),
            pltpu.VMEM((2 * total * block, 4 * limbs * block), jnp.bfloat16),
            jax.ShapeDtypeStruct((limbs, block, width * count), jnp.float32),
        ]
        + [pltpu.VMEM((limbs // 2, block, width), jnp.int32)] * peers,
        scratch_shapes=[
            pltpu.VMEM((count, limbs, block, width), jnp.float32),
            pltpu.VMEM((limbs, block, width), jnp.float32),
            pltpu.SMEM(levels.shape, jnp.int32),
            pltpu.SMEM(moduli.shape, jnp.int32),
            pltpu.VMEM(cross.shape, jnp.int32),
            pltpu.SemaphoreType.DMA((count,)),
            pltpu.SemaphoreType.DMA((width // tile_of(width),)),
            pltpu.SemaphoreType.DMA((3,)),
        ],
        compiler_params=params(14),
        cost_estimate=cost(peers * limbs * block * width, 16, 6 * peers * limbs * block * width),
        name="pack",
    )(place, columns, *(far(x) for x in (levels, moduli, cross, residues)))
    return *results[:3], dict(zip(offsets[1:], results[3:]))


def scale_kernel(chunk, relay, emit, place, columns, targets, *rest):
    offsets, low, high = chunk
    values, rest = rest[: len(offsets)], rest[len(offsets) :]
    if relay:
        outer, arrived, *rest = rest
    if emit:
        source, scaled, *rest = rest[1:]
        stage, sems = rest[-2:]
    else:
        scaled, *rest = rest
    send = rest[0] if relay else None
    width = values[0].shape[2]
    length = high - low
    tile = tile_of(length)
    steps = length // tile
    inner = (place[0] == 1) | (place[0] == 2)
    stores = []
    for turn, offset in enumerate(offsets):
        start = (place[1] ^ offset) * width + low

        def store(step, turn=turn, start=start):
            return out_copy(stage.at[turn], source, start, step, tile, sems.at[turn])

        def body(step):
            write = pl.ds(pl.multiple_of(turn * length + step * tile, tile), tile)
            read = pl.ds(pl.multiple_of(low + step * tile, tile), tile)
            local = span_of(step, tile)
            scale_tile(values[turn], columns, stage.at[turn] if emit else None, scaled, read, write, local)
            if relay:
                for word in range(send.shape[0]):
                    words = scaled[word, :, write]
                    if word < outer.shape[0]:
                        words = jnp.where(inner, relay_word(targets, outer, arrived, word, write), words)
                    send[word, :, write] = words
            if emit:
                store(step).start()

        loop(steps, body)
        stores.append(store)
    if emit:
        for store in stores:
            loop(steps, lambda step: store(step).wait())


def scale_chunk(place, columns, targets, values, chunk, source, relay=None):
    words, block, _ = values[0].shape
    _, low, high = chunk
    length = high - low
    parts = len(values)
    limbs = 2 * words
    emit = source is not None
    operands = [place, columns, targets, *values, *(relay or ())]
    in_specs = [SCALARS] + [HERE] * (len(operands) - 1)
    whole = pltpu.VMEM((words, block, length * parts), jnp.int32)
    out_shape, out_specs, scratch, aliases = [whole], [HERE], [], {}
    if relay:
        out_shape, out_specs = out_shape + [whole], out_specs + [HERE]
    if emit:
        aliases = {len(operands): 0}
        operands.append(source)
        in_specs.append(FAR)
        out_shape = [jax.ShapeDtypeStruct(source.shape, jnp.float32)] + out_shape
        out_specs = [FAR] + out_specs
        scratch = [
            pltpu.VMEM((parts, limbs, block, length), jnp.float32),
            pltpu.SemaphoreType.DMA((parts, length // tile_of(length))),
        ]
    results = pl.pallas_call(
        functools.partial(scale_kernel, chunk, relay is not None, emit),
        in_specs=in_specs,
        out_specs=out_specs,
        out_shape=out_shape,
        scratch_shapes=scratch,
        input_output_aliases=aliases,
        compiler_params=params(8),
        cost_estimate=cost(parts * limbs * block * length, 40, 8 * parts * limbs * block * length),
        name="scale",
    )(*operands)
    if emit:
        source, *results = results
    scaled = results[0]
    return source, scaled, results[1] if relay else scaled


def spread_kernel(pieces, place, columns, *rest):
    values = rest[: len(pieces)]
    source, stage, sems = rest[-3:]
    tile = stage.shape[3]
    stores = []
    for turn, (offset, low, high, width) in enumerate(pieces):
        steps = (high - low) // tile
        base = sum((p[2] - p[1]) // tile for p in pieces[:turn])

        def store(step, base=base, offset=offset, low=low, width=width):
            return pltpu.make_async_copy(
                stage.at[base + step],
                source.at[:, :, pl.ds(pl.multiple_of((place[1] ^ offset) * width + low + step * tile, tile), tile)],
                sems.at[base + step],
            )

        def body(step):
            read = pl.ds(pl.multiple_of(low + step * tile, tile), tile)
            for word in range(values[turn].shape[0]):
                for side, value in enumerate(halves(values[turn][word, :, read])):
                    limb = 2 * word + side
                    stage[base + step, limb] = value.astype(jnp.float32) * spread(columns[2, limb], tile)
            store(step).start()

        loop(steps, body)
        stores.append((steps, store))
    for steps, store in stores:
        loop(steps, lambda step: store(step).wait())


def spread_blocks(place, columns, values, pieces, source):
    words, block, width = values[0].shape
    tile = min(tile_of(high - low) for _, low, high in pieces)
    pieces = tuple((offset, low, high, width) for offset, low, high in pieces)
    slots = sum((high - low) // tile for _, low, high, _ in pieces)
    operands = [place, columns, *values, source]
    return pl.pallas_call(
        functools.partial(spread_kernel, pieces),
        in_specs=[SCALARS] + [HERE] * (len(operands) - 2) + [FAR],
        out_specs=FAR,
        out_shape=jax.ShapeDtypeStruct(source.shape, jnp.float32),
        scratch_shapes=[
            pltpu.VMEM((slots, 2 * words, block, tile), jnp.float32),
            pltpu.SemaphoreType.DMA((slots,)),
        ],
        input_output_aliases={len(operands) - 1: 0},
        compiler_params=params(12),
        cost_estimate=cost(slots * 2 * words * block * tile, 20, 6 * slots * 2 * words * block * tile),
        name="spread",
    )(*operands)


def mix_kernel(targets, weights, own, received, *outs):
    block = own.shape[1]
    tile = min(own.shape[2], 2048)

    def body(step):
        span = span_of(step, tile)
        digits = []
        for words in (own, received):
            for word in range(words.shape[0]):
                value = words[word, :, span]
                for byte in range(4):
                    part = lax.shift_right_logical(value, 8 * byte) if byte else value
                    if byte < 3:
                        part = part & 0xFF
                    digits.append(part.astype(jnp.float32))
        stacked = jnp.concatenate(digits, axis=0).astype(jnp.bfloat16)
        sums = jnp.dot(weights[...], stacked, preferred_element_type=jnp.float32)
        reduced = []
        for target in range(targets.shape[1]):
            modulus, inverse = spread(targets[0, target], tile), spread(targets[1, target], tile)
            low = sums[2 * target * block : (2 * target + 1) * block]
            high = sums[(2 * target + 1) * block : (2 * target + 2) * block]
            upper = centred(high, modulus, inverse)
            reduced.append(residue(256.0 * upper + low, modulus, inverse).astype(jnp.int32))
        words = [pack_pair(reduced[t], reduced[t + 1]) for t in range(0, len(reduced), 2)]
        position = 0
        for out in outs:
            for word in range(out.shape[0]):
                out[word, :, span] = words[position]
                position += 1

    loop(own.shape[2] // tile, body)


def mix_chunk(own, received, weights, targets, split):
    words, block, length = own.shape
    total = targets.shape[1]
    part = total // 8
    counts = (part, part, part, part) if split else (2 * part, part, part)
    return pl.pallas_call(
        mix_kernel,
        in_specs=[HERE] * 4,
        out_specs=[HERE] * len(counts),
        out_shape=[pltpu.VMEM((count, block, length), jnp.int32) for count in counts],
        compiler_params=params(8),
        cost_estimate=cost(total * block * length, 40, 4 * (2 * words + 4) * block * length),
        name="mix",
    )(targets, weights, own, received)


def relay_word(targets, outer, arrived, word, span):
    words = outer.shape[0]
    results = []
    for side, (a, b) in enumerate(zip(halves(outer[word, :, span]), halves(arrived[words + word, :, span]))):
        modulus = spread(targets[0, 4 * words + 2 * word + side].astype(jnp.int32), span.size)
        results.append(join_residues(a, b, modulus))
    return pack_pair(*results)


def forward_kernel(targets, outer, arrived, out):
    tile = tile_of(out.shape[2])

    def body(step):
        span = span_of(step, tile)
        for word in range(out.shape[0]):
            out[word, :, span] = relay_word(targets, outer, arrived, word, span)

    loop(out.shape[2] // tile, body)


def forward_chunk(outer, arrived, targets):
    words, block, length = outer.shape
    return pl.pallas_call(
        forward_kernel,
        in_specs=[HERE] * 3,
        out_specs=HERE,
        out_shape=pltpu.VMEM(outer.shape, jnp.int32),
        compiler_params=params(4),
        cost_estimate=cost(words * block * length, 40, 12 * words * block * length),
        name="forward",
    )(targets, outer, arrived)


def finish_kernel(chunks, full, widths, place, targets, *rest):
    out, stage, sems = rest[-3:]
    tile = stage.shape[3]
    inner = (place[0] == 1) | (place[0] == 2)
    stores = []
    slot = 0
    position = 0
    for turn, (offsets, low, high) in enumerate(chunks):
        mine, arrived, relayed, *direct = rest[position : position + widths[turn]]
        position += widths[turn]
        first_target = 6 * mine.shape[0]
        steps = (high - low) // tile
        for part, offset in enumerate(offsets):

            def store(step, offset=offset, low=low, base=slot):
                start = (place[1] ^ offset) * full + low
                return pltpu.make_async_copy(
                    stage.at[base + step],
                    out.at[:, :, pl.ds(pl.multiple_of(start + step * tile, tile), tile)],
                    sems.at[base + step],
                )

            def body(step):
                span = pl.ds(pl.multiple_of(part * (high - low) + step * tile, tile), tile)
                for word in range(mine.shape[0]):
                    other = jnp.where(inner, arrived[word, :, span], relayed[word, :, span])
                    parts = [halves(mine[word, :, span]), halves(other)]
                    parts += [halves(jnp.where(inner, 0, more[word, :, span])) for more in direct]
                    for side, (total, *terms) in enumerate(zip(*parts)):
                        target = first_target + 2 * word + side
                        modulus = spread(targets[0, target].astype(jnp.int32), tile)
                        for term in terms:
                            total = join_residues(total, term, modulus)
                        total = total.astype(jnp.float32)
                        stage[slot + step, 2 * word + side] = total * spread(targets[1, target], tile)
                store(step).start()

            loop(steps, body)
            stores.append((steps, store))
            slot += steps
    for steps, store in stores:
        loop(steps, lambda step: store(step).wait())


def finish_chunks(place, targets, triples, chunks, shape, full, buffer):
    words, block, _ = triples[0][0].shape
    tile = min(tile_of(high - low) for _, low, high in chunks)
    slots = sum(len(offsets) * (high - low) // tile for offsets, low, high in chunks)
    operands = [place, targets, *(array for triple in triples for array in triple)]
    in_specs = [SCALARS] + [HERE] * (len(operands) - 1)
    aliases = {}
    if buffer is not None:
        aliases[len(operands)] = 0
        operands.append(buffer)
        in_specs.append(FAR)
    return pl.pallas_call(
        functools.partial(finish_kernel, chunks, full, [len(triple) for triple in triples]),
        in_specs=in_specs,
        out_specs=FAR,
        out_shape=jax.ShapeDtypeStruct(shape, jnp.float32),
        scratch_shapes=[
            pltpu.VMEM((slots, 2 * words, block, tile), jnp.float32),
            pltpu.SemaphoreType.DMA((slots,)),
        ],
        input_output_aliases=aliases,
        compiler_params=params(8),
        cost_estimate=cost(2 * words * block * slots * tile, 20, 10 * 2 * words * block * slots * tile),
        name="finish",
    )(*operands)


def chunk_plan(count, width):
    if count == 8:
        return [((offset,), 0, width) for offset in (0, 1, 2, 4, 3, 5, 6, 7)]
    unit = max(1, count // 8)
    edges = sorted({0, 1} | set(range(unit, count + 1, unit)))
    return [(tuple(range(start, end)), 0, width) for start, end in zip(edges, edges[1:])]


LAG = 3
LATE = 4


def length_of(chunk):
    return len(chunk[0]) * (chunk[2] - chunk[1])


def riders(plan):
    return {
        step: step - LAG
        for step in range(LAG, len(plan))
        if length_of(plan[step]) == length_of(plan[step - LAG])
    }


def timeline(plan):
    steps = len(plan)
    ride = riders(plan)
    events = ["first", "a0", "pack"]
    order = list(dict.fromkeys(offset for chunk in plan for offset in chunk[0] if offset))
    ready = list(dict.fromkeys(offset for chunk in plan[:4] for offset in chunk[0] if offset))
    events += [f"p{offset}" for offset in ready]
    events += ["scale1", "a1"] + [f"p{offset}" for offset in order if offset not in ready]
    alone = [step for step in range(steps) if step not in ride.values()]
    for step in range(steps):
        events += [f"mix{step}", f"b{step}"]
        if step == steps - 1:
            events += [f"d{step}", f"c{step}"]
        if step + 2 < steps:
            events += [f"scale{step + 2}", f"a{step + 2}"]
        if step - 1 in alone:
            events += [f"forward{step - 1}", f"c{step - 1}"]
    joined = [step for step in range(steps) if step not in alone]
    tail = steps - 1
    events[events.index(f"c{tail}") + 1 : events.index(f"c{tail}") + 1] = ["spread"]
    events += ["finish" + "_".join(map(str, joined + alone[:-2])), f"finish{tail - 1}", f"finish{tail}"]
    return events


def late(plan):
    return set(range(len(plan) - LATE, len(plan)))


def per_device(residues, levels, moduli, inverse_table, cross_table):
    target_count = cross_table.shape[2]
    _, _, width = residues.shape
    count = lax.axis_size("coef")
    assert lax.axis_size("limb") == 4
    block = residues.shape[1] // count
    place = jnp.stack([lax.axis_index("limb"), lax.axis_index("coef")]).astype(jnp.int32)
    cross = jnp.transpose(cross_table, (0, 2, 1))
    plan = chunk_plan(count, width)
    steps = len(plan)
    ride = riders(plan)

    scaled, send, received, mixed, crossed, relayed = ([None] * steps for _ in range(6))
    arrived = {}
    result = None
    shape = (target_count // 4, block, width * count)
    for event in timeline(plan):
        kind = event.rstrip("0123456789_")
        step = int(event[len(kind) :] or 0) if "_" not in event else 0
        if kind == "first":
            columns, scaled[0] = first(place, levels, moduli, inverse_table, residues, block, plan[0][2])
            send[0] = scaled[0]
        elif kind == "pack":
            targets, weights, source, packed = pack_blocks(
                place, columns, levels, moduli, cross, residues, block, count
            )
        elif kind == "p":
            arrived[step] = lax.ppermute(packed[step], "coef", [(i, i ^ step) for i in range(count)])
        elif kind == "scale":
            values = [arrived[offset] for offset in plan[step][0]]
            relay = (mixed[ride[step]][1], crossed[ride[step]]) if step in ride else None
            buffer = None if step in late(plan) else source
            buffer, scaled[step], send[step] = scale_chunk(place, columns, targets, values, plan[step], buffer, relay)
            source = source if step in late(plan) else buffer
        elif kind == "a":
            pairs = [(0, 1), (3, 2)] + ([(1, 0), (2, 3)] if step in ride else [])
            received[step] = lax.ppermute(send[step], "limb", pairs)
            if step in ride:
                relayed[ride[step]] = received[step]
        elif kind == "mix":
            mixed[step] = mix_chunk(scaled[step], received[step], weights, targets, step == steps - 1)
        elif kind == "b":
            crossed[step] = lax.ppermute(mixed[step][0], "limb", [(1, 2), (2, 1)])
        elif kind == "forward":
            relayed[step] = forward_chunk(mixed[step][1], crossed[step], targets)
        elif kind == "c":
            share = mixed[step][2] if step == steps - 1 else relayed[step]
            relayed[step] = lax.ppermute(share, "limb", [(1, 0), (2, 3)])
        elif kind == "d":
            direct = lax.ppermute(mixed[step][1], "limb", [(1, 3), (2, 0)])
        elif kind == "spread":
            pieces = [(offset, low, high) for i in sorted(late(plan)) for offset, low, high in [(o, *plan[i][1:]) for o in plan[i][0]]]
            source = spread_blocks(place, columns, [arrived[p[0]] for p in pieces], pieces, source)
        else:
            chosen = [int(i) for i in event[len(kind) :].split("_")]
            triples = [(mixed[i][-1], crossed[i], relayed[i]) for i in chosen]
            if chosen[-1] == steps - 1:
                triples[-1] += (direct,)
            result = finish_chunks(
                place, targets, triples, tuple(plan[i] for i in chosen), shape, width, result
            )
    return (source, result)


def solution(mesh):
    placed = (P("limb", None, "coef"), P(), P(), P(), P())

    return jax.shard_map(
        per_device,
        mesh=mesh,
        in_specs=placed,
        out_specs=(P("limb", "coef", None), P("limb", "coef", None)),
        check_vma=False,
    )
```

```python
import functools

import jax
import jax.numpy as jnp
from jax import lax
from jax.experimental import pallas as pl
from jax.experimental.pallas import tpu as pltpu
from jax.sharding import PartitionSpec as P

LANES = 128
MIB = 1024 * 1024
HERE = pl.BlockSpec(memory_space=pltpu.VMEM)
FAR = pl.BlockSpec(memory_space=pl.ANY)
SCALARS = pl.BlockSpec(memory_space=pltpu.SMEM)


def log2(number):
    assert number & (number - 1) == 0
    return number.bit_length() - 1


def pack_pair(first, second):
    return first | lax.shift_left(second, 16)


def halves(word):
    return word & 0xFFFF, lax.shift_right_logical(word, 16)


def centred(amount, modulus, inverse):
    return amount - jnp.round(amount * inverse) * modulus


def residue(amount, modulus, inverse):
    remain = centred(amount, modulus, inverse)
    return jnp.where(remain < 0, remain + modulus, remain)


def join_residues(first, second, modulus):
    total = first + second
    less = total - modulus
    return jnp.where(less < 0, total, less)


def spread(column, width):
    return jnp.concatenate([column] * (width // LANES), axis=1)


def params(limit):
    return pltpu.CompilerParams(vmem_limit_bytes=limit * MIB)


def cost(elements, ops, moved):
    return pl.CostEstimate(flops=elements * ops, bytes_accessed=moved, transcendentals=0)


def loop(count, body):
    lax.fori_loop(0, count, lambda step, carry: (body(step), carry)[1], 0)


def span_of(step, tile):
    return pl.ds(pl.multiple_of(step * tile, tile), tile)


def constants(limit):
    return lambda number: jnp.full(limit, number, jnp.int32).astype(jnp.float32)


def product(left, right):
    return jnp.dot(left, right, preferred_element_type=jnp.float32)


def bytes_of(table):
    parts = (table & 0xFF, lax.shift_right_logical(table, 8))
    return [part.astype(jnp.float32).astype(jnp.bfloat16) for part in parts]


def level_rows(place, levels, block, source_count):
    lane = lax.broadcasted_iota(jnp.int32, (block, source_count), 1)
    rank = lax.broadcasted_iota(jnp.int32, (block, source_count), 0)
    level_rank = jnp.zeros((block, source_count), jnp.int32)
    for n in range(block):
        level_rank = jnp.where(rank == n, levels[place[1] * block + n] - 1, level_rank)
    return lane, level_rank, jnp.where(lane == level_rank, 1.0, 0.0).astype(jnp.bfloat16)


def build_columns(place, levels, moduli, inverse, columns):
    group = place[0]
    limbs, block = columns.shape[1], columns.shape[2]
    lane, level_rank, onehot = level_rows(place, levels, block, inverse.shape[0])
    inverse_low, inverse_high = (product(onehot, part) for part in bytes_of(inverse[...]))
    inverse_rows = jnp.where(lane <= level_rank, inverse_low + 256.0 * inverse_high, 0.0)
    live_rows = jnp.where(lane <= level_rank, 1.0, 0.0)
    shape = (block, LANES)
    fill = constants(shape)
    for limb in range(limbs):
        index = group * limbs + limb
        here = lane == index
        picked = jnp.sum(jnp.where(here, inverse_rows, 0.0), axis=1, keepdims=True)
        picked = jnp.broadcast_to(picked, shape)
        live = jnp.broadcast_to(jnp.sum(jnp.where(here, live_rows, 0.0), axis=1, keepdims=True), shape)
        high = jnp.floor((picked + 128.0) * (1.0 / 256.0))
        modulus = fill(moduli[index])
        columns[0, limb] = high
        columns[1, limb] = picked - 256.0 * high
        columns[2, limb] = live / modulus
        columns[3, limb] = modulus
        columns[4, limb] = 1.0 / modulus


def build_weights(place, levels, moduli, cross, limbs, targets, weights):
    group = place[0]
    total, block = targets.shape[1:3]
    source_count = cross.shape[0]
    quarter = total // 4
    fill = constants((block, LANES))
    onehot = level_rows(place, levels, block, source_count)[2]
    left = group < 2
    inner = (group == 1) | (group == 2)
    order = (jnp.where(left, 2, 1), jnp.where(left, 3, 0), group ^ 1, group)
    rows = []
    for target in range(total):
        index = order[target // quarter] * quarter + target % quarter
        rows += [product(onehot, part) for part in bytes_of(cross[:, index, :])]
    width = weights.shape[1]
    entry = lax.broadcasted_iota(jnp.int32, (source_count, width), 0)
    column = lax.broadcasted_iota(jnp.int32, (source_count, width), 1)
    received = lax.shift_right_logical(column, log2(2 * block * limbs))
    limb = lax.shift_right_logical(column, log2(2 * block)) & (limbs - 1)
    limb = limb + jnp.where(received == 0, group * limbs, (group ^ 1) * limbs)
    choose = jnp.where(entry == limb, 1.0, 0.0).astype(jnp.bfloat16)
    chosen = product(jnp.concatenate(rows, axis=0).astype(jnp.bfloat16), choose)
    column = lax.broadcasted_iota(jnp.int32, (block, width), 1)
    same = (column & (block - 1)) == lax.broadcasted_iota(jnp.int32, (block, width), 0)
    upper = (lax.shift_right_logical(column, log2(block)) & 1) == 1
    from_outer = lax.shift_right_logical(column, log2(2 * block * limbs)) == 1
    results = []
    for target in range(total):
        index = order[target // quarter] * quarter + target % quarter
        modulus = fill(moduli[source_count + index])
        inverse_modulus = 1.0 / modulus
        targets[0, target] = modulus
        targets[1, target] = inverse_modulus
        modulus, inverse_modulus = spread(modulus, width), spread(inverse_modulus, width)
        first = 2 * target * block
        value = chosen[first : first + block] + 256.0 * chosen[first + block : first + 2 * block]
        value = jnp.where(upper, residue(256.0 * value, modulus, inverse_modulus), value)
        use = jnp.where(inner, 1, 0) if target // quarter != 2 else 0
        value = jnp.where(same & ((from_outer == False) | (use > 0)), value, 0.0)
        high_byte = jnp.floor(value * (1.0 / 256.0))
        results += [value - 256.0 * high_byte, high_byte]
    weights[...] = jnp.concatenate(results, axis=0).astype(jnp.bfloat16)


def scale_tile(values, columns, scaled, read, write):
    width = write.size
    for word in range(scaled.shape[0]):
        if values.dtype == jnp.int32:
            pair = halves(values[word, :, read])
        else:
            pair = (values[2 * word, :, read], values[2 * word + 1, :, read])
        results = []
        for side, value in enumerate(pair):
            value = value.astype(jnp.float32)
            high, low, _, modulus, inverse = (spread(columns[kind, 2 * word + side], width) for kind in range(5))
            upper = centred(value * high, modulus, inverse)
            results.append(residue(256.0 * upper + value * low, modulus, inverse).astype(jnp.int32))
        scaled[word, :, write] = pack_pair(*results)


def first_kernel(place, *rest):
    tables, residues, scaled, landing, columns = rest[:3], *rest[3:7]
    copies, (sems, table_sems) = rest[7:-2], rest[-2:]
    block, width = landing.shape[1:]
    tile = width // sems.shape[0]

    def load(step):
        return pltpu.make_async_copy(
            residues.at[:, pl.ds(pl.multiple_of(place[1] * block, block), block), span_of(step, tile)],
            landing.at[:, :, span_of(step, tile)],
            sems.at[step],
        )

    @pl.when((place[0] != 1) & (place[0] != 2))
    def _():
        steps = width // tile
        fetches = [pltpu.make_async_copy(a, b, table_sems.at[i]) for i, (a, b) in enumerate(zip(tables, copies))]
        for fetch in fetches:
            fetch.start()
        loop(steps, lambda step: load(step).start())
        for fetch in fetches:
            fetch.wait()
        build_columns(place, *copies, columns)

        def body(step):
            load(step).wait()
            span = span_of(step, tile)
            scale_tile(landing, columns, scaled, span, span)

        loop(steps, body)


def tile_of(width, most=1024):
    return next(tile for tile in range(min(width, most), 0, -LANES) if width % tile == 0)


def first(place, levels, moduli, inverse_table, residues, block, length):
    limbs = residues.shape[0]
    steps = length // tile_of(length)
    return pl.pallas_call(
        first_kernel,
        in_specs=[SCALARS] + [FAR] * 4,
        out_specs=HERE,
        out_shape=pltpu.VMEM((limbs // 2, block, length), jnp.int32),
        scratch_shapes=[
            pltpu.VMEM((limbs, block, length), jnp.float32),
            pltpu.VMEM((5, limbs, block, LANES), jnp.float32),
            pltpu.SMEM(levels.shape, jnp.int32),
            pltpu.SMEM(moduli.shape, jnp.int32),
            pltpu.VMEM(inverse_table.shape, jnp.int32),
            pltpu.SemaphoreType.DMA((steps,)),
            pltpu.SemaphoreType.DMA((3,)),
        ],
        compiler_params=params(8),
        cost_estimate=cost(limbs * block * length, 60, 10 * limbs * block * length),
        name="first",
    )(place, *(far(x) for x in (levels, moduli, inverse_table, residues)))


def far(array):
    return pltpu.with_memory_space_constraint(array, pltpu.HBM)


def pack_kernel(offsets, tables, place, residues, *rest):
    if tables:
        arrays, rest = rest[:4], rest[4:]
        columns, targets, weights, scaled, *rest = rest
        *rest, level_copy, moduli_copy, inverse_copy, cross_copy, table_sems = rest
        copies = (level_copy, moduli_copy, inverse_copy, cross_copy)
    *outs, landing, sems = rest
    _, limbs, block, width = landing.shape
    tile = tile_of(width)

    def load(turn):
        peer = place[1] ^ offsets[turn]
        return pltpu.make_async_copy(
            residues.at[:, pl.ds(pl.multiple_of(peer * block, block), block), :], landing.at[turn], sems.at[turn]
        )

    if tables:
        fetches = [pltpu.make_async_copy(a, b, table_sems.at[i]) for i, (a, b) in enumerate(zip(arrays, copies))]
        for fetch in fetches:
            fetch.start()
    for turn in range(len(offsets)):
        load(turn).start()
    if tables:
        for fetch in fetches:
            fetch.wait()
        build_columns(place, level_copy, moduli_copy, inverse_copy, columns)
        build_weights(place, level_copy, moduli_copy, cross_copy, limbs, targets, weights)
    for turn, out in enumerate(outs):
        load(turn).wait()

        def body(step):
            span = span_of(step, tile)
            for word in range(limbs // 2):
                one = landing[turn, 2 * word, :, span].astype(jnp.int32)
                two = landing[turn, 2 * word + 1, :, span].astype(jnp.int32)
                out[word, :, span] = pack_pair(one, two)
            if offsets[turn] == 0:
                scale_tile(landing.at[turn], columns, scaled, span, span)

        loop(width // tile, body)


def pack_blocks(place, residues, offsets, block, tables=()):
    limbs, _, width = residues.shape
    blocks = len(offsets)
    words = pltpu.VMEM((limbs // 2, block, width), jnp.int32)
    shapes, scratch = [], []
    if tables:
        levels, moduli, inverse_table, cross = tables
        total = cross.shape[1]
        shapes = [
            pltpu.VMEM((5, limbs, block, LANES), jnp.float32),
            pltpu.VMEM((2, total, block, LANES), jnp.float32),
            pltpu.VMEM((2 * total * block, 4 * limbs * block), jnp.bfloat16),
            words,
        ]
        scratch = [
            pltpu.SMEM(levels.shape, jnp.int32),
            pltpu.SMEM(moduli.shape, jnp.int32),
            pltpu.VMEM(inverse_table.shape, jnp.int32),
            pltpu.VMEM(cross.shape, jnp.int32),
            pltpu.SemaphoreType.DMA((4,)),
        ]
    results = pl.pallas_call(
        functools.partial(pack_kernel, offsets, bool(tables)),
        in_specs=[SCALARS] + [FAR] * (1 + len(tables)),
        out_specs=[HERE] * (len(shapes) + blocks),
        out_shape=shapes + [words] * blocks,
        scratch_shapes=[
            pltpu.VMEM((blocks, limbs, block, width), jnp.float32),
            pltpu.SemaphoreType.DMA((blocks,)),
        ]
        + scratch,
        compiler_params=params(10),
        cost_estimate=cost(blocks * limbs * block * width, 16, 6 * blocks * limbs * block * width),
        name="pack",
    )(place, *(far(x) for x in (residues, *tables)))
    return results[: len(shapes)], dict(zip(offsets, results[len(shapes) :]))


def scale_kernel(chunk, relay, place, columns, targets, *rest):
    offsets, low, high = chunk
    values, rest = rest[: len(offsets)], rest[len(offsets) :]
    if relay:
        outer, arrived, scaled, send = rest
    else:
        (scaled,) = rest
    length = high - low
    tile = tile_of(length)
    inner = (place[0] == 1) | (place[0] == 2)
    for turn in range(len(offsets)):

        def body(step):
            write = pl.ds(pl.multiple_of(turn * length + step * tile, tile), tile)
            read = pl.ds(pl.multiple_of(low + step * tile, tile), tile)
            scale_tile(values[turn], columns, scaled, read, write)
            if relay:
                for word in range(send.shape[0]):
                    words = scaled[word, :, write]
                    if word < outer.shape[0]:
                        words = jnp.where(inner, relay_word(targets, outer, arrived, word, write), words)
                    send[word, :, write] = words

        loop(length // tile, body)


def scale_chunk(place, columns, targets, values, chunk, relay=None):
    words, block, _ = values[0].shape
    parts = len(values)
    length = parts * (chunk[2] - chunk[1])
    operands = [place, columns, targets, *values, *(relay or ())]
    count = 2 if relay else 1
    results = pl.pallas_call(
        functools.partial(scale_kernel, chunk, relay is not None),
        in_specs=[SCALARS] + [HERE] * (len(operands) - 1),
        out_specs=[HERE] * count,
        out_shape=[pltpu.VMEM((words, block, length), jnp.int32)] * count,
        compiler_params=params(4),
        cost_estimate=cost(2 * words * block * length, 40, 16 * words * block * length),
        name="scale",
    )(*operands)
    return results[0], results[-1]


def spread_kernel(pieces, place, columns, *rest):
    values = rest[: len(pieces)]
    source, stage, sems = rest[-3:]
    tile = stage.shape[3]
    stores = []
    for turn, (offset, low, high, width) in enumerate(pieces):
        steps = (high - low) // tile
        base = sum((p[2] - p[1]) // tile for p in pieces[:turn])

        def store(step, base=base, offset=offset, low=low, width=width):
            return pltpu.make_async_copy(
                stage.at[base + step],
                source.at[:, :, pl.ds(pl.multiple_of((place[1] ^ offset) * width + low + step * tile, tile), tile)],
                sems.at[base + step],
            )

        def body(step):
            read = pl.ds(pl.multiple_of(low + step * tile, tile), tile)
            for word in range(values[turn].shape[0]):
                for side, value in enumerate(halves(values[turn][word, :, read])):
                    limb = 2 * word + side
                    stage[base + step, limb] = value.astype(jnp.float32) * spread(columns[2, limb], tile)
            store(step).start()

        loop(steps, body)
        stores.append((steps, store))
    for steps, store in stores:
        loop(steps, lambda step: store(step).wait())


def spread_blocks(place, columns, values, offsets, shape, buffer):
    words, block, width = values[0].shape
    tile = tile_of(width)
    pieces = tuple((offset, 0, width, width) for offset in offsets)
    slots = len(pieces) * (width // tile)
    operands = [place, columns, *values]
    in_specs = [SCALARS] + [HERE] * (len(operands) - 1)
    aliases = {}
    if buffer is not None:
        aliases[len(operands)] = 0
        operands.append(buffer)
        in_specs.append(FAR)
    return pl.pallas_call(
        functools.partial(spread_kernel, pieces),
        in_specs=in_specs,
        out_specs=FAR,
        out_shape=jax.ShapeDtypeStruct(shape, jnp.float32),
        scratch_shapes=[
            pltpu.VMEM((slots, 2 * words, block, tile), jnp.float32),
            pltpu.SemaphoreType.DMA((slots,)),
        ],
        input_output_aliases=aliases,
        compiler_params=params(10),
        cost_estimate=cost(slots * 2 * words * block * tile, 20, 6 * slots * 2 * words * block * tile),
        name="spread",
    )(*operands)


def mix_kernel(first_target, targets, weights, own, received, *outs):
    block = own.shape[1]
    tile = tile_of(own.shape[2], 2048)
    count = 2 * sum(out.shape[0] for out in outs)
    rows = pl.ds(2 * first_target * block, 2 * count * block)

    def body(step):
        span = span_of(step, tile)
        digits = []
        for words in (own, received):
            for word in range(words.shape[0]):
                value = words[word, :, span]
                for byte in range(4):
                    part = lax.shift_right_logical(value, 8 * byte) if byte else value
                    if byte < 3:
                        part = part & 0xFF
                    digits.append(part.astype(jnp.float32))
        stacked = jnp.concatenate(digits, axis=0).astype(jnp.bfloat16)
        sums = product(weights[rows, :], stacked)
        reduced = []
        for target in range(count):
            modulus = spread(targets[0, first_target + target], tile)
            inverse = spread(targets[1, first_target + target], tile)
            low = sums[2 * target * block : (2 * target + 1) * block]
            high = sums[(2 * target + 1) * block : (2 * target + 2) * block]
            upper = centred(high, modulus, inverse)
            reduced.append(residue(256.0 * upper + low, modulus, inverse).astype(jnp.int32))
        words = [pack_pair(reduced[t], reduced[t + 1]) for t in range(0, count, 2)]
        position = 0
        for out in outs:
            for word in range(out.shape[0]):
                out[word, :, span] = words[position]
                position += 1

    loop(own.shape[2] // tile, body)


def mix_chunk(own, received, weights, targets, near):
    words, block, length = own.shape
    total = targets.shape[1]
    counts = (total // 8, total // 8) if near else (total // 4,)
    return pl.pallas_call(
        functools.partial(mix_kernel, total // 2 if near else 0),
        in_specs=[HERE] * 4,
        out_specs=[HERE] * len(counts),
        out_shape=[pltpu.VMEM((count, block, length), jnp.int32) for count in counts],
        compiler_params=params(8),
        cost_estimate=cost(total * block * length, 20, 4 * (2 * words + 2) * block * length),
        name="near" if near else "far",
    )(targets, weights, own, received)


def relay_word(targets, outer, arrived, word, span):
    words = outer.shape[0]
    results = []
    for side, (a, b) in enumerate(zip(halves(outer[word, :, span]), halves(arrived[words + word, :, span]))):
        modulus = spread(targets[0, 4 * words + 2 * word + side].astype(jnp.int32), span.size)
        results.append(join_residues(a, b, modulus))
    return pack_pair(*results)


def forward_kernel(targets, outer, arrived, out):
    tile = tile_of(out.shape[2])

    def body(step):
        span = span_of(step, tile)
        for word in range(out.shape[0]):
            out[word, :, span] = relay_word(targets, outer, arrived, word, span)

    loop(out.shape[2] // tile, body)


def forward_chunk(outer, arrived, targets):
    words, block, length = outer.shape
    return pl.pallas_call(
        forward_kernel,
        in_specs=[HERE] * 3,
        out_specs=HERE,
        out_shape=pltpu.VMEM(outer.shape, jnp.int32),
        compiler_params=params(4),
        cost_estimate=cost(words * block * length, 40, 12 * words * block * length),
        name="forward",
    )(targets, outer, arrived)


def finish_kernel(chunks, full, place, targets, *rest):
    out, stage, sems = rest[-3:]
    tile = stage.shape[3]
    inner = (place[0] == 1) | (place[0] == 2)
    stores = []
    slot = 0
    for turn, (offsets, low, high) in enumerate(chunks):
        mine, arrived, relayed = rest[3 * turn : 3 * turn + 3]
        first_target = 6 * mine.shape[0]
        steps = (high - low) // tile
        for part, offset in enumerate(offsets):

            def store(step, offset=offset, low=low, base=slot):
                start = (place[1] ^ offset) * full + low
                return pltpu.make_async_copy(
                    stage.at[base + step],
                    out.at[:, :, pl.ds(pl.multiple_of(start + step * tile, tile), tile)],
                    sems.at[base + step],
                )

            def body(step):
                span = pl.ds(pl.multiple_of(part * (high - low) + step * tile, tile), tile)
                for word in range(mine.shape[0]):
                    other = jnp.where(inner, arrived[word, :, span], relayed[word, :, span])
                    parts = [halves(mine[word, :, span]), halves(other)]
                    for side, (a, b) in enumerate(zip(*parts)):
                        target = first_target + 2 * word + side
                        modulus = spread(targets[0, target].astype(jnp.int32), tile)
                        total = join_residues(a, b, modulus).astype(jnp.float32)
                        stage[slot + step, 2 * word + side] = total * spread(targets[1, target], tile)
                store(step).start()

            loop(steps, body)
            stores.append((steps, store))
            slot += steps
    for steps, store in stores:
        loop(steps, lambda step: store(step).wait())


def finish_chunks(place, targets, triples, chunks, shape, full, buffer):
    words, block, _ = triples[0][0].shape
    tile = min(tile_of(high - low) for _, low, high in chunks)
    slots = sum(len(offsets) * (high - low) // tile for offsets, low, high in chunks)
    operands = [place, targets, *(array for triple in triples for array in triple)]
    in_specs = [SCALARS] + [HERE] * (len(operands) - 1)
    aliases = {}
    if buffer is not None:
        aliases[len(operands)] = 0
        operands.append(buffer)
        in_specs.append(FAR)
    return pl.pallas_call(
        functools.partial(finish_kernel, chunks, full),
        in_specs=in_specs,
        out_specs=FAR,
        out_shape=jax.ShapeDtypeStruct(shape, jnp.float32),
        scratch_shapes=[
            pltpu.VMEM((slots, 2 * words, block, tile), jnp.float32),
            pltpu.SemaphoreType.DMA((slots,)),
        ],
        input_output_aliases=aliases,
        compiler_params=params(8),
        cost_estimate=cost(2 * words * block * slots * tile, 20, 10 * 2 * words * block * slots * tile),
        name="finish",
    )(*operands)


def chunk_plan(count, width):
    if count == 8:
        order = [(offset,) for offset in (0, 1, 2, 4, 3, 5, 6, 7)]
    else:
        unit = max(1, count // 8)
        edges = sorted({0, 1} | set(range(unit, count + 1, unit)))
        order = [tuple(range(start, end)) for start, end in zip(edges, edges[1:])]
    cut = 5 * width // 8
    plan = [(offsets, 0, width) for offsets in order]
    if cut % LANES == 0:
        plan[-1:] = [(order[-1], 0, cut), (order[-1], cut, width)]
    return plan


LAG = 3


def length_of(chunk):
    return len(chunk[0]) * (chunk[2] - chunk[1])


def riders(plan):
    return {
        step: step - LAG
        for step in range(LAG, len(plan))
        if length_of(plan[step]) == length_of(plan[step - LAG])
    }


def name_of(kind, numbers):
    return kind + "_".join(map(str, numbers))


def peers_of(chunks):
    return list(dict.fromkeys(offset for chunk in chunks for offset in chunk[0] if offset))


def timeline(plan):
    steps = len(plan)
    alone = [step for step in range(steps) if step not in riders(plan).values()]
    soon, later = peers_of(plan[:4]), peers_of(plan[4:])
    later = [offset for offset in later if offset not in soon]
    middle = [offset for offset in peers_of(plan[:6]) if offset not in soon]
    blocks = [0] + peers_of(plan)
    quarter = -(-len(blocks) // 4)
    groups = [blocks[start : start + quarter] for start in range(0, len(blocks), quarter)]
    fill = {3: [name_of("spread", groups[0])], 4: [name_of("spread", groups[1])]}
    fill |= {5: [name_of("finish", [0, 1])], 6: [name_of("spread", groups[2])], 7: [name_of("finish", [2, 3])]}
    events = ["first", "a0", "packa"] + [f"p{offset}" for offset in soon] + ["packb"]
    events += [f"p{offset}" for offset in middle] + ["scale1", "a1"]
    for step in range(steps):
        events += [f"far{step}", f"b{step}", f"near{step}"]
        if step == 0:
            events += [f"p{offset}" for offset in later if offset not in middle]
        if step == steps - 1:
            events += [name_of("spread", group) for group in groups[3:]]
        if step + 2 < steps:
            events += [f"scale{step + 2}", f"a{step + 2}"]
        if step - 1 in alone:
            events += [f"forward{step - 1}", f"c{step - 1}"]
        events += fill.get(step, [])
    last = steps - 1
    events += [name_of("finish", range(4, last - 1)), f"forward{last}", f"c{last}"]
    events += [name_of("finish", [last - 1, last])]
    return events


def per_device(residues, levels, moduli, inverse_table, cross_table):
    target_count = cross_table.shape[2]
    limbs, _, width = residues.shape
    count = lax.axis_size("coef")
    assert lax.axis_size("limb") == 4
    block = residues.shape[1] // count
    place = jnp.stack([lax.axis_index("limb"), lax.axis_index("coef")]).astype(jnp.int32)
    cross = jnp.transpose(cross_table, (0, 2, 1))
    plan = chunk_plan(count, width)
    steps = len(plan)
    ride = riders(plan)

    scaled, send, received, far_sums, near_sums, crossed, relayed = ([None] * steps for _ in range(7))
    arrived = {}
    source, result = None, None
    source_shape = (limbs, block, width * count)
    shape = (target_count // 4, block, width * count)
    soon = tuple(peers_of(plan[:4]))
    for event in timeline(plan):
        kind = event.rstrip("0123456789_")
        numbers = [int(number) for number in event[len(kind) :].split("_") if number]
        step = numbers[0] if numbers else 0
        if kind == "first":
            send[0] = first(place, levels, moduli, inverse_table, residues, block, plan[0][2])
        elif kind == "packa":
            packed = pack_blocks(place, residues, soon, block)[1]
        elif kind == "packb":
            others = tuple(offset for offset in range(count) if offset not in soon)
            tables = (levels, moduli, inverse_table, cross)
            (columns, targets, weights, scaled[0]), more = pack_blocks(place, residues, others, block, tables)
            packed |= more
            arrived[0] = packed[0]
        elif kind == "p":
            arrived[step] = lax.ppermute(packed[step], "coef", [(i, i ^ step) for i in range(count)])
        elif kind == "scale":
            values = [arrived[offset] for offset in plan[step][0]]
            relay = (near_sums[ride[step]][0], crossed[ride[step]]) if step in ride else None
            scaled[step], send[step] = scale_chunk(place, columns, targets, values, plan[step], relay)
        elif kind == "a":
            pairs = [(0, 1), (3, 2)] + ([(1, 0), (2, 3)] if step in ride else [])
            received[step] = lax.ppermute(send[step], "limb", pairs)
            if step in ride:
                relayed[ride[step]] = received[step]
        elif kind == "far":
            (far_sums[step],) = mix_chunk(scaled[step], received[step], weights, targets, False)
        elif kind == "near":
            near_sums[step] = mix_chunk(scaled[step], received[step], weights, targets, True)
        elif kind == "b":
            crossed[step] = lax.ppermute(far_sums[step], "limb", [(1, 2), (2, 1)])
        elif kind == "forward":
            relayed[step] = forward_chunk(near_sums[step][0], crossed[step], targets)
        elif kind == "c":
            relayed[step] = lax.ppermute(relayed[step], "limb", [(1, 0), (2, 3)])
        elif kind == "spread":
            values = [arrived[offset] for offset in numbers]
            source = spread_blocks(place, columns, values, numbers, source_shape, source)
        else:
            triples = [(near_sums[i][1], crossed[i], relayed[i]) for i in numbers]
            chunks = tuple(plan[i] for i in numbers)
            result = finish_chunks(place, targets, triples, chunks, shape, width, result)
    return (source, result)


def solution(mesh):
    placed = (P("limb", None, "coef"), P(), P(), P(), P())

    return jax.shard_map(
        per_device,
        mesh=mesh,
        in_specs=placed,
        out_specs=(P("limb", "coef", None), P("limb", "coef", None)),
        check_vma=False,
    )
```
